32 devices in a mesh: gx: 4 (over z), gy: 2 (over y), gz: 4 (over x, core).
Axes of the slice: x: 2, y: 2, z: 4, core: 2. Of those that a mesh axis runs over, the one named last changes fastest.
Arguments:
- hidden_acts: bfloat16 [4, 2, 4, 256, 16384], P('gz', 'gy', 'gx'), may hold values from -6 to 6
- output_grad: bfloat16 [4, 2, 4, 256, 32], P('gz', 'gy', 'gx'), may hold values from -6 to 6
- weights: bfloat16 [4, 2, 4, 32, 16384], P('gz', 'gy', 'gx'), may hold values from -6 to 6
- momentum: bfloat16 [4, 2, 4, 32, 16384], P('gz', 'gy', 'gx'), may hold values from -48 to 48
- worker_of_slot: int32 [32], replicated, may hold values from 0 to 31, each once
- round_shift: int32 [8], replicated, may hold values from 0 to 4, as said below
Outputs:
- mixed: bfloat16 [4, 2, 4, 32, 16384], P('gx', 'gy', 'gz')
- new_momentum: bfloat16 [4, 2, 4, 32, 16384], P('gz', 'gy', 'gx')
The draws below stay inside these ranges and needn't reach their ends.
Inputs may be any that keep to these rules, and one draw needn't show every extreme that they name: `round_shift`: each entry is below log2 of 32, so offsets are powers of two below 32; some round has offset 32 / 2 and some round offset 1.
All inputs are finite; a program needn't handle non-finite values.
Results may differ from the reference program's by a relative error of at most 0.0081.
Values may be sent and summed in bfloat16 or wider, within the bound.
A program may use at most 64 MiB of HBM per device.

```python
import jax
import jax.numpy as jnp
from jax import lax

FF = 16384
ROWS = 32
TOK = 256
ROUNDS = 8
WORKERS = 32
N_GX = 4
N_GY = 2
N_GZ = 4


def draw_round_shift(key, part):
    levels = WORKERS.bit_length() - 1
    first_key = jax.random.fold_in(key, 11)
    second_key = jax.random.fold_in(key, 23)
    values = jax.random.randint(first_key, (ROUNDS,), 0, levels, dtype=jnp.int32)
    order = jax.random.permutation(second_key, ROUNDS)
    values = values.at[order[0]].set(jnp.int32(levels - 1))
    values = values.at[order[1]].set(jnp.int32(0))
    return values.astype(jnp.int32)


def shard_levels(rng, shape, split, least, top_value):
    def one(position, shards_of):
        heights = jax.random.uniform(jax.random.fold_in(jax.random.fold_in(rng, 6), position), (shards_of,), jnp.float32, least / len(split), top_value / len(split))
        return jnp.repeat(jnp.exp(heights), shape[position] // shards_of).reshape((-1,) + (1,) * (len(shape) - position - 1))

    level = one(*split[0])
    for cut in split[1:]:
        level = level * one(*cut)
    return level


def scatter_about(key, extent, deviation, most, cuts=(), kind=jnp.bfloat16):
    entries = deviation * jax.random.normal(key, extent, jnp.float32)
    if cuts:
        entries = entries * shard_levels(key, extent, cuts, -0.22, 0.18)
    return jnp.clip(entries, -most, most).astype(kind)


def setup_inputs(seed: int = 0) -> dict:
    seeds = jax.random.split(jax.random.key(seed), 7)
    return {
        "hidden_acts": scatter_about(seeds[0], (N_GZ, N_GY, N_GX, TOK, FF), 1.0, 6.0, ((0, 4), (1, 2), (2, 4))),
        "output_grad": scatter_about(seeds[1], (N_GZ, N_GY, N_GX, TOK, ROWS), 1.0, 6.0, ((0, 4), (1, 2), (2, 4))),
        "weights": scatter_about(seeds[2], (N_GZ, N_GY, N_GX, ROWS, FF), 1.0, 6.0, ((0, 4), (1, 2), (2, 4))),
        "momentum": scatter_about(seeds[3], (N_GZ, N_GY, N_GX, ROWS, FF), 8.0, 48.0, ((0, 4), (1, 2), (2, 4))),
        "worker_of_slot": jax.random.permutation(seeds[4], WORKERS).astype(jnp.int32),
        "round_shift": draw_round_shift(jax.random.fold_in(seeds[6], 71), 0),
    }


learn_rate = 0.01
beta_keep = 0.9


def local_step(items):
    hidden, grad_out, weight, moment = items
    grad = lax.dot_general(grad_out, hidden, (((0,), (0,)), ((), ())), preferred_element_type=jnp.float32)
    velocity = beta_keep * moment.astype(jnp.float32) + grad
    stepped = (weight.astype(jnp.float32) - learn_rate * velocity).astype(jnp.bfloat16)
    return stepped, velocity.astype(jnp.bfloat16)


def reference(hidden_acts, output_grad, weights, momentum, worker_of_slot, round_shift):
    workers = N_GX * N_GY * N_GZ
    hidden = hidden_acts.reshape(workers, TOK, FF)
    grad_out = output_grad.reshape(workers, TOK, ROWS)
    weight = weights.reshape(workers, ROWS, FF)
    moment = momentum.reshape(workers, ROWS, FF)
    stepped, new_moment = lax.map(local_step, (hidden, grad_out, weight, moment))
    replica = jnp.zeros_like(stepped).at[worker_of_slot].set(stepped)
    for step in range(ROUNDS):
        offset = jnp.left_shift(jnp.int32(1), round_shift[step].astype(jnp.int32))
        peer = jnp.roll(replica, offset, axis=0)
        replica = ((replica.astype(jnp.float32) + peer.astype(jnp.float32)) * 0.5).astype(jnp.bfloat16)
    mixed = replica.reshape(N_GX, N_GY, N_GZ, ROWS, FF)
    return mixed, new_moment.reshape(N_GZ, N_GY, N_GX, ROWS, FF)
```

```python
import functools

import jax
import jax.numpy as jnp
from jax import lax
from jax.experimental import pallas as pl
from jax.experimental.pallas import tpu as pltpu
from jax.sharding import PartitionSpec as P

learn_rate = 0.01
beta_keep = 0.9
TILE = 16
GROUP = 2
LOGICAL = pl.DeviceIdType.LOGICAL


def iota(shape, axis):
    return lax.broadcasted_iota(jnp.int32, shape, axis)


def ones_where(mask):
    return jnp.where(mask, 1.0, 0.0).astype(jnp.bfloat16)


def exact_dot(a, b):
    return jnp.dot(a, b, preferred_element_type=jnp.float32)


def kernel(
    sizes,
    hidden_hbm,
    grad_hbm,
    weight_hbm,
    moment_hbm,
    held_hbm,
    shift_hbm,
    out_ref,
    new_moment_ref,
    hidden,
    grad_ref,
    weight,
    moment,
    held_ref,
    shift_ref,
    stage,
    recv,
    mixed,
    spread,
    load_sem,
    grad_sem,
    table_sem,
    send_sem,
    recv_sem,
    back_send_sem,
    back_recv_sem,
):
    size_x, size_y, size_z = sizes
    workers = size_x * size_y * size_z
    width = stage.shape[-1]
    groups, _, span = hidden.shape
    columns = stage.shape[1]
    parts = out_ref.shape[0] // TILE
    chunks = recv.shape[0]
    rounds = shift_ref.shape[0]
    my_x, my_y, my_z = lax.axis_index("gx"), lax.axis_index("gy"), lax.axis_index("gz")
    me = (my_x * size_y + my_y) * size_z + my_z
    slot = my_x + size_x * (my_y + size_y * my_z)

    plane = size_y * size_z
    half = workers // 2
    side = lax.div(me, half)

    def target(step):
        return me ^ (workers - 1 - step)

    def ranked(step):
        far = 1 - lax.div(step, half)
        turn = (side ^ far) * (size_x - 1)
        layer = lax.div(lax.rem(step, half), plane) ^ turn
        return layer * plane + ((me & (plane - 1)) ^ (plane - 1 - lax.rem(step, plane)))

    def column(step):
        return ranked(step) if columns == workers else (me ^ (columns - 1 - step)) & (columns - 1)

    def pair(group):
        return lax.div(column(group * GROUP), GROUP)

    def loads(group):
        place = pair(group)
        cut = pl.ds(pl.multiple_of(place * span, 128), span)
        return [
            pltpu.make_async_copy(source.at[:, cut], kept.at[place], load_sem.at[group])
            for source, kept in (
                (hidden_hbm, hidden),
                (moment_hbm, moment),
                (weight_hbm, weight),
            )
        ]

    def load(group, carry):
        for copy in loads(group):
            copy.start()
        return carry

    barrier = pltpu.get_barrier_semaphore()

    def greet(step, carry):
        pl.semaphore_signal(
            barrier, inc=1, device_id=target(step), device_id_type=LOGICAL
        )
        return carry

    grad_copy = pltpu.make_async_copy(grad_hbm, grad_ref, grad_sem.at[0])
    table_copies = [
        pltpu.make_async_copy(held_hbm, held_ref, table_sem.at[0]),
        pltpu.make_async_copy(shift_hbm, shift_ref, table_sem.at[1]),
    ]
    grad_copy.start()
    load(0, 0)
    lax.fori_loop(0, workers - 1, greet, 0)
    lax.fori_loop(1, groups, load, 0)
    for copy in table_copies:
        copy.start()

    def place_of(part, where):
        block = part * columns
        return block // workers, block % workers + where

    def send(part, where):
        chunk, device = place_of(part, where)

        @pl.when(device != me)
        def _():
            pltpu.make_async_remote_copy(
                src_ref=stage.at[part, where],
                dst_ref=recv.at[chunk, slot],
                send_sem=send_sem.at[chunk],
                recv_sem=recv_sem.at[chunk],
                device_id=device,
                device_id_type=LOGICAL,
            ).start()

    early = [part for part in range(parts) if place_of(part, 0)[0] == 0]
    late = [part for part in range(parts) if place_of(part, 0)[0] > 0]

    def compute(group):
        place = pair(group)
        for copy in loads(group):
            copy.wait()
        grad = exact_dot(grad_ref[...], hidden[place])
        velocity = beta_keep * moment[place].astype(jnp.float32) + grad
        cut = pl.ds(pl.multiple_of(place * span, 128), span)
        new_moment_ref[:, cut] = velocity.astype(jnp.bfloat16)
        stepped = (weight[place].astype(jnp.float32) - learn_rate * velocity).astype(
            jnp.bfloat16
        )
        for k in range(GROUP):
            for part in range(parts):
                stage[part, place * GROUP + k] = stepped[
                    part * TILE : (part + 1) * TILE, k * width : (k + 1) * width
                ]

    def send_early(group):
        for k in range(GROUP):
            for part in early:
                send(part, column(group * GROUP + k))

    def compute_and_send(group, carry):
        compute(group)
        send_early(group - 1)
        return carry

    grad_copy.wait()
    compute(jnp.int32(0))
    pl.semaphore_wait(barrier, workers - 1)
    send_early(jnp.int32(0))
    compute(jnp.int32(1))
    lax.fori_loop(2, groups, compute_and_send, 0)
    send_early(jnp.int32(groups - 1))
    for part in late:
        lax.fori_loop(0, columns, lambda step, c: (send(part, column(step)), c)[1], 0)
    for chunk in range(chunks):
        block = chunk * workers + me
        recv[chunk, slot] = stage[lax.div(block, columns), lax.rem(block, columns)]
    for copy in table_copies:
        copy.wait()

    square = (workers, workers)
    gap = lax.rem(iota(square, 0) - iota(square, 1) + workers, workers)
    level = jnp.full(square, -1, jnp.int32)
    for power in range(workers.bit_length() - 1):
        level = jnp.where(gap == 1 << power, power, level)
    table = ones_where(held_ref[...] == iota(square, 0))
    for step in range(rounds):
        turn = ones_where((gap == 0) | (level == shift_ref[step]))
        table = exact_dot(turn, table).astype(jnp.bfloat16)
    distinct = workers // 2
    table = (table[:distinct].astype(jnp.float32) * 0.5**rounds).astype(jnp.bfloat16)
    wide = (workers, workers * TILE)
    table = exact_dot(table, ones_where(iota(wide, 1) // TILE == iota(wide, 0))).astype(
        jnp.bfloat16
    )
    height = min(256, distinct * TILE)

    def fill(step, carry):
        tall = (height, distinct)
        pick = ones_where((iota(tall, 0) + step * height) // TILE == iota(tall, 1))
        full = (height, workers * TILE)
        same = iota(full, 0) % TILE == iota(full, 1) % TILE
        spread[pl.ds(pl.multiple_of(step * height, height), height), :] = jnp.where(
            same, exact_dot(pick, table), 0.0
        ).astype(jnp.bfloat16)
        return carry

    lax.fori_loop(0, distinct * TILE // height, fill, 0)

    def pieces_wait(sem):
        ref = recv.at[0, pl.ds(0, workers - 1)]
        pltpu.make_async_copy(ref, ref, sem).wait()

    for chunk in range(chunks):
        pieces_wait(recv_sem.at[chunk])
        got = recv[chunk].reshape(workers * TILE, width)

        def blend(step, carry):
            result = exact_dot(
                spread[pl.ds(pl.multiple_of(step * height, height), height), :], got
            )
            mixed[chunk, pl.ds(step * (height // TILE), height // TILE)] = result.astype(
                jnp.bfloat16
            ).reshape(height // TILE, TILE, width)
            return carry

        lax.fori_loop(0, distinct * TILE // height, blend, 0)
        block = chunk * workers + me
        row = pl.multiple_of(lax.div(block, columns) * TILE, TILE)
        first = pl.multiple_of(lax.rem(block, columns) * width, 128)
        mine = (pl.ds(row, TILE), pl.ds(first, width))
        out_ref[mine] = mixed[chunk, lax.rem(me, distinct)]

        turned = workers // 2 if chunk == chunks - 1 else 0

        def back(step, carry):
            device = ranked(lax.rem(step + turned, workers))

            @pl.when(device != me)
            def _():
                pltpu.make_async_remote_copy(
                    src_ref=mixed.at[chunk, lax.rem(device, distinct)],
                    dst_ref=out_ref.at[mine],
                    send_sem=back_send_sem.at[chunk],
                    recv_sem=back_recv_sem.at[chunk],
                    device_id=device,
                    device_id_type=LOGICAL,
                ).start()

            return carry

        lax.fori_loop(0, workers, back, 0)

    for chunk in range(chunks):
        pieces_wait(send_sem.at[chunk])
        pieces_wait(back_send_sem.at[chunk])
        pieces_wait(back_recv_sem.at[chunk])


def store(mixed_ref, moment_ref, mixed_hbm, moment_hbm, sem):
    copies = [
        pltpu.make_async_copy(mixed_ref, mixed_hbm, sem.at[0]),
        pltpu.make_async_copy(moment_ref, moment_hbm, sem.at[1]),
    ]
    for copy in copies:
        copy.start()
    for copy in copies:
        copy.wait()


def shards(sizes, hidden_acts, output_grad, weights, momentum, worker_of_slot, round_shift):
    hidden = hidden_acts.reshape(hidden_acts.shape[-2:])
    grad_out = output_grad.reshape(output_grad.shape[-2:]).T
    weight = weights.reshape(weights.shape[-2:])
    moment = momentum.reshape(momentum.shape[-2:])
    workers = sizes[0] * sizes[1] * sizes[2]
    tokens, features = hidden.shape
    rows = weight.shape[0]
    parts = rows // TILE
    width = max(128, features // workers)
    columns = features // width
    chunks = parts * columns // workers
    distinct = workers // 2
    groups = columns // GROUP
    anywhere = pl.BlockSpec(memory_space=pl.ANY)
    vmem = pl.BlockSpec(memory_space=pltpu.VMEM)
    half = jnp.bfloat16
    mixed, new_moment = pl.pallas_call(
        functools.partial(kernel, sizes),
        out_shape=[pltpu.VMEM((rows, features), half)] * 2,
        in_specs=[anywhere] * 6,
        out_specs=[vmem, vmem],
        scratch_shapes=[
            pltpu.VMEM((groups, tokens, GROUP * width), half),
            pltpu.VMEM((rows, tokens), half),
            pltpu.VMEM((groups, rows, GROUP * width), half),
            pltpu.VMEM((groups, rows, GROUP * width), half),
            pltpu.VMEM((1, workers), jnp.int32),
            pltpu.SMEM(round_shift.shape, jnp.int32),
            pltpu.VMEM((parts, columns, TILE, width), half),
            pltpu.VMEM((chunks, workers, TILE, width), half),
            pltpu.VMEM((chunks, distinct, TILE, width), half),
            pltpu.VMEM((distinct * TILE, workers * TILE), half),
            pltpu.SemaphoreType.DMA((groups,)),
            pltpu.SemaphoreType.DMA((1,)),
            pltpu.SemaphoreType.DMA((2,)),
            pltpu.SemaphoreType.DMA((chunks,)),
            pltpu.SemaphoreType.DMA((chunks,)),
            pltpu.SemaphoreType.DMA((chunks,)),
            pltpu.SemaphoreType.DMA((chunks,)),
        ],
        compiler_params=pltpu.CompilerParams(
            collective_id=0, has_side_effects=True, vmem_limit_bytes=60 * 1024 * 1024
        ),
        name="step_and_gossip",
    )(hidden, grad_out, weight, moment, worker_of_slot.reshape(1, workers), round_shift)
    mixed, new_moment = pl.pallas_call(
        store,
        out_shape=[jax.ShapeDtypeStruct((rows, features), half)] * 2,
        in_specs=[anywhere, anywhere],
        out_specs=[anywhere, anywhere],
        scratch_shapes=[pltpu.SemaphoreType.DMA((2,))],
        name="store",
    )(
        pltpu.with_memory_space_constraint(mixed, pltpu.VMEM),
        pltpu.with_memory_space_constraint(new_moment, pltpu.VMEM),
    )
    return (mixed.reshape(weights.shape), new_moment.reshape(momentum.shape))


def solution(mesh):
    sizes = (mesh.shape["gx"], mesh.shape["gy"], mesh.shape["gz"])
    placed = (
        P("gz", "gy", "gx", None, None),
        P("gz", "gy", "gx", None, None),
        P("gz", "gy", "gx", None, None),
        P("gz", "gy", "gx", None, None),
        P(),
        P(),
    )
    return jax.shard_map(
        functools.partial(shards, sizes),
        mesh=mesh,
        in_specs=placed,
        out_specs=(P("gx", "gy", "gz", None, None), P("gz", "gy", "gx", None, None)),
        check_vma=False,
    )
```

```python
import functools

import jax
import jax.numpy as jnp
from jax import lax
from jax.experimental import pallas as pl
from jax.experimental.pallas import tpu as pltpu
from jax.sharding import PartitionSpec as P

learn_rate = 0.01
beta_keep = 0.9
TILE = 16
GROUP = 2
LOGICAL = pl.DeviceIdType.LOGICAL


def iota(shape, axis):
    return lax.broadcasted_iota(jnp.int32, shape, axis)


def ones_where(mask):
    return jnp.where(mask, 1.0, 0.0).astype(jnp.bfloat16)


def exact_dot(a, b):
    return jnp.dot(a, b, preferred_element_type=jnp.float32)


def kernel(
    sizes,
    hidden_hbm,
    grad_hbm,
    weight_hbm,
    moment_hbm,
    held_hbm,
    shift_hbm,
    out_ref,
    new_moment_ref,
    hidden,
    grad_ref,
    weight,
    moment,
    held_ref,
    shift_ref,
    stage,
    recv,
    mixed,
    spread,
    load_sem,
    grad_sem,
    table_sem,
    hub_sem,
    all_sem,
    send_sem,
    recv_sem,
    back_send_sem,
    back_recv_sem,
):
    size_x, size_y, size_z = sizes
    workers = size_x * size_y * size_z
    width = stage.shape[-1]
    groups, _, span = hidden.shape
    columns = stage.shape[1]
    parts = out_ref.shape[0] // TILE
    chunks = recv.shape[0]
    rounds = shift_ref.shape[0]
    my_x, my_y, my_z = lax.axis_index("gx"), lax.axis_index("gy"), lax.axis_index("gz")
    me = (my_x * size_y + my_y) * size_z + my_z
    slot = my_x + size_x * (my_y + size_y * my_z)

    plane = size_y * size_z
    half = workers // 2
    side = lax.div(me, half)
    lines = plane // GROUP
    layers = (half if columns == workers else columns) // plane
    my_line = lax.div(lax.rem(me, plane), GROUP)

    def ranked(step):
        far = 1 - lax.div(step, half)
        turn = (side ^ far) * (size_x - 1)
        layer = lax.div(lax.rem(step, half), plane) ^ turn
        return layer * plane + ((me & (plane - 1)) ^ (plane - 1 - lax.rem(step, plane)))

    def pair(group):
        side_groups = layers * lines
        order = lax.rem(group, side_groups)
        turn = my_line ^ ((lines - lax.div(order, layers)) & (lines - 1))
        layer = lax.rem(order, layers)
        if columns == workers:
            layer = layer ^ ((side ^ (1 - lax.div(group, side_groups))) * (size_x - 1))
        return layer * lines + turn

    def loads(group):
        place = pair(group)
        cut = pl.ds(pl.multiple_of(place * span, 128), span)
        return [
            pltpu.make_async_copy(source.at[:, cut], kept.at[place], load_sem.at[group])
            for source, kept in (
                (hidden_hbm, hidden),
                (moment_hbm, moment),
                (weight_hbm, weight),
            )
        ]

    def load(group, carry):
        for copy in loads(group):
            copy.start()
        return carry

    barrier = pltpu.get_barrier_semaphore()
    hub = my_x == 0

    def signal(sem, device):
        pl.semaphore_signal(sem, inc=1, device_id=device, device_id_type=LOGICAL)

    mates = size_x * GROUP - 1

    def greet(step, carry):
        mate = mates - step
        signal(barrier, me ^ (lax.div(mate, GROUP) * plane + lax.rem(mate, GROUP)))
        return carry

    def greet_hub(step, carry):
        signal(barrier, me ^ ((step + 1) * GROUP))
        return carry

    def tell_hub(step, carry):
        signal(hub_sem, me ^ ((step + 1) * GROUP))
        return carry

    def tell_line(step, carry):
        signal(all_sem, me + (step + 1) * plane)
        return carry

    grad_copy = pltpu.make_async_copy(grad_hbm, grad_ref, grad_sem.at[0])
    table_copies = [
        pltpu.make_async_copy(held_hbm, held_ref, table_sem.at[0]),
        pltpu.make_async_copy(shift_hbm, shift_ref, table_sem.at[1]),
    ]
    grad_copy.start()
    load(0, 0)
    lax.fori_loop(0, mates, greet, 0)

    @pl.when(hub)
    def _():
        lax.fori_loop(0, lines - 1, greet_hub, 0)
    lax.fori_loop(1, groups, load, 0)
    for copy in table_copies:
        copy.start()

    def place_of(part, where):
        block = part * columns
        return block // workers, block % workers + where

    def send(part, where):
        chunk, device = place_of(part, where)

        @pl.when(device != me)
        def _():
            pltpu.make_async_remote_copy(
                src_ref=stage.at[part, where],
                dst_ref=recv.at[chunk, slot],
                send_sem=send_sem.at[chunk],
                recv_sem=recv_sem.at[chunk],
                device_id=device,
                device_id_type=LOGICAL,
            ).start()

    early = [part for part in range(parts) if place_of(part, 0)[0] == 0]
    late = [part for part in range(parts) if place_of(part, 0)[0] > 0]

    def compute(group):
        place = pair(group)
        for copy in loads(group):
            copy.wait()
        grad = exact_dot(grad_ref[...], hidden[place])
        velocity = beta_keep * moment[place].astype(jnp.float32) + grad
        cut = pl.ds(pl.multiple_of(place * span, 128), span)
        new_moment_ref[:, cut] = velocity.astype(jnp.bfloat16)
        stepped = (weight[place].astype(jnp.float32) - learn_rate * velocity).astype(
            jnp.bfloat16
        )
        for k in range(GROUP):
            for part in range(parts):
                stage[part, place * GROUP + k] = stepped[
                    part * TILE : (part + 1) * TILE, k * width : (k + 1) * width
                ]

    def send_parts(which, group):
        for k in range(GROUP):
            for part in which:
                send(part, pair(group) * GROUP + k)

    def compute_ahead(group, carry):
        compute(group)
        return carry

    def send_ahead(group, carry):
        send_parts(early, group)
        return carry

    def compute_and_send(group, carry):
        compute(group)
        send_parts(early, group - 1)
        return carry

    def send_late(group, carry):
        send_parts(late, group)
        return carry

    grad_copy.wait()
    compute(jnp.int32(0))
    pl.semaphore_wait(barrier, mates + jnp.where(hub, lines - 1, 0))

    @pl.when(hub)
    def _():
        lax.fori_loop(0, lines - 1, tell_hub, 0)

    send_parts(early, jnp.int32(0))
    for group in range(1, layers):
        compute(jnp.int32(group))
        send_parts(early, jnp.int32(group))
    for group in range(layers):
        send_parts(late, jnp.int32(group))
    ahead = min(layers + 4, groups - 1)
    lax.fori_loop(layers, ahead, compute_ahead, 0)

    @pl.when(hub)
    def _():
        pl.semaphore_wait(hub_sem, lines - 1)
        lax.fori_loop(0, size_x - 1, tell_line, 0)

    @pl.when(jnp.logical_not(hub))
    def _():
        pl.semaphore_wait(all_sem, 1)

    lax.fori_loop(layers, ahead - 1, send_ahead, 0)
    lax.fori_loop(ahead, groups, compute_and_send, 0)
    send_parts(early, jnp.int32(groups - 1))
    if late:
        lax.fori_loop(layers, groups, send_late, 0)
    for chunk in range(chunks):
        block = chunk * workers + me
        recv[chunk, slot] = stage[lax.div(block, columns), lax.rem(block, columns)]
    for copy in table_copies:
        copy.wait()

    square = (workers, workers)
    gap = lax.rem(iota(square, 0) - iota(square, 1) + workers, workers)
    level = jnp.full(square, -1, jnp.int32)
    for power in range(workers.bit_length() - 1):
        level = jnp.where(gap == 1 << power, power, level)
    table = ones_where(held_ref[...] == iota(square, 0))
    for step in range(rounds):
        turn = ones_where((gap == 0) | (level == shift_ref[step]))
        table = exact_dot(turn, table).astype(jnp.bfloat16)
    distinct = workers // 2
    table = (table[:distinct].astype(jnp.float32) * 0.5**rounds).astype(jnp.bfloat16)
    wide = (workers, workers * TILE)
    table = exact_dot(table, ones_where(iota(wide, 1) // TILE == iota(wide, 0))).astype(
        jnp.bfloat16
    )
    height = min(256, distinct * TILE)

    def fill(step, carry):
        tall = (height, distinct)
        pick = ones_where((iota(tall, 0) + step * height) // TILE == iota(tall, 1))
        full = (height, workers * TILE)
        same = iota(full, 0) % TILE == iota(full, 1) % TILE
        spread[pl.ds(pl.multiple_of(step * height, height), height), :] = jnp.where(
            same, exact_dot(pick, table), 0.0
        ).astype(jnp.bfloat16)
        return carry

    lax.fori_loop(0, distinct * TILE // height, fill, 0)

    def pieces_wait(sem):
        ref = recv.at[0, pl.ds(0, workers - 1)]
        pltpu.make_async_copy(ref, ref, sem).wait()

    for chunk in range(chunks):
        pieces_wait(recv_sem.at[chunk])
        got = recv[chunk].reshape(workers * TILE, width)

        def blend(step, carry):
            result = exact_dot(
                spread[pl.ds(pl.multiple_of(step * height, height), height), :], got
            )
            mixed[chunk, pl.ds(step * (height // TILE), height // TILE)] = result.astype(
                jnp.bfloat16
            ).reshape(height // TILE, TILE, width)
            return carry

        lax.fori_loop(0, distinct * TILE // height, blend, 0)
        block = chunk * workers + me
        row = pl.multiple_of(lax.div(block, columns) * TILE, TILE)
        first = pl.multiple_of(lax.rem(block, columns) * width, 128)
        mine = (pl.ds(row, TILE), pl.ds(first, width))
        out_ref[mine] = mixed[chunk, lax.rem(me, distinct)]

        turned = workers // 2 if chunk == chunks - 1 else 0

        def back(step, carry):
            device = ranked(lax.rem(step + turned, workers))

            @pl.when(device != me)
            def _():
                pltpu.make_async_remote_copy(
                    src_ref=mixed.at[chunk, lax.rem(device, distinct)],
                    dst_ref=out_ref.at[mine],
                    send_sem=back_send_sem.at[chunk],
                    recv_sem=back_recv_sem.at[chunk],
                    device_id=device,
                    device_id_type=LOGICAL,
                ).start()

            return carry

        lax.fori_loop(0, workers, back, 0)

    for chunk in range(chunks):
        pieces_wait(send_sem.at[chunk])
        pieces_wait(back_send_sem.at[chunk])
        pieces_wait(back_recv_sem.at[chunk])


def store(mixed_ref, moment_ref, mixed_hbm, moment_hbm, sem):
    copies = [
        pltpu.make_async_copy(mixed_ref, mixed_hbm, sem.at[0]),
        pltpu.make_async_copy(moment_ref, moment_hbm, sem.at[1]),
    ]
    for copy in copies:
        copy.start()
    for copy in copies:
        copy.wait()


def shards(sizes, hidden_acts, output_grad, weights, momentum, worker_of_slot, round_shift):
    hidden = hidden_acts.reshape(hidden_acts.shape[-2:])
    grad_out = output_grad.reshape(output_grad.shape[-2:]).T
    weight = weights.reshape(weights.shape[-2:])
    moment = momentum.reshape(momentum.shape[-2:])
    workers = sizes[0] * sizes[1] * sizes[2]
    tokens, features = hidden.shape
    rows = weight.shape[0]
    parts = rows // TILE
    width = max(128, features // workers)
    columns = features // width
    chunks = parts * columns // workers
    distinct = workers // 2
    groups = columns // GROUP
    anywhere = pl.BlockSpec(memory_space=pl.ANY)
    vmem = pl.BlockSpec(memory_space=pltpu.VMEM)
    half = jnp.bfloat16
    mixed, new_moment = pl.pallas_call(
        functools.partial(kernel, sizes),
        out_shape=[pltpu.VMEM((rows, features), half)] * 2,
        in_specs=[anywhere] * 6,
        out_specs=[vmem, vmem],
        scratch_shapes=[
            pltpu.VMEM((groups, tokens, GROUP * width), half),
            pltpu.VMEM((rows, tokens), half),
            pltpu.VMEM((groups, rows, GROUP * width), half),
            pltpu.VMEM((groups, rows, GROUP * width), half),
            pltpu.VMEM((1, workers), jnp.int32),
            pltpu.SMEM(round_shift.shape, jnp.int32),
            pltpu.VMEM((parts, columns, TILE, width), half),
            pltpu.VMEM((chunks, workers, TILE, width), half),
            pltpu.VMEM((chunks, distinct, TILE, width), half),
            pltpu.VMEM((distinct * TILE, workers * TILE), half),
            pltpu.SemaphoreType.DMA((groups,)),
            pltpu.SemaphoreType.DMA((1,)),
            pltpu.SemaphoreType.DMA((2,)),
            pltpu.SemaphoreType.REGULAR,
            pltpu.SemaphoreType.REGULAR,
            pltpu.SemaphoreType.DMA((chunks,)),
            pltpu.SemaphoreType.DMA((chunks,)),
            pltpu.SemaphoreType.DMA((chunks,)),
            pltpu.SemaphoreType.DMA((chunks,)),
        ],
        compiler_params=pltpu.CompilerParams(
            collective_id=0, has_side_effects=True, vmem_limit_bytes=60 * 1024 * 1024
        ),
        name="step_and_gossip",
    )(hidden, grad_out, weight, moment, worker_of_slot.reshape(1, workers), round_shift)
    mixed, new_moment = pl.pallas_call(
        store,
        out_shape=[jax.ShapeDtypeStruct((rows, features), half)] * 2,
        in_specs=[anywhere, anywhere],
        out_specs=[anywhere, anywhere],
        scratch_shapes=[pltpu.SemaphoreType.DMA((2,))],
        name="store",
    )(
        pltpu.with_memory_space_constraint(mixed, pltpu.VMEM),
        pltpu.with_memory_space_constraint(new_moment, pltpu.VMEM),
    )
    return (mixed.reshape(weights.shape), new_moment.reshape(momentum.shape))


def solution(mesh):
    sizes = (mesh.shape["gx"], mesh.shape["gy"], mesh.shape["gz"])
    placed = (
        P("gz", "gy", "gx", None, None),
        P("gz", "gy", "gx", None, None),
        P("gz", "gy", "gx", None, None),
        P("gz", "gy", "gx", None, None),
        P(),
        P(),
    )
    return jax.shard_map(
        functools.partial(shards, sizes),
        mesh=mesh,
        in_specs=placed,
        out_specs=(P("gx", "gy", "gz", None, None), P("gz", "gy", "gx", None, None)),
        check_vma=False,
    )
```

```python
import functools

import jax
import jax.numpy as jnp
from jax import lax
from jax.experimental import pallas as pl
from jax.experimental.pallas import tpu as pltpu
from jax.sharding import PartitionSpec as P

learn_rate = 0.01
beta_keep = 0.9
TILE = 16
GROUP = 2
LOGICAL = pl.DeviceIdType.LOGICAL


def iota(shape, axis):
    return lax.broadcasted_iota(jnp.int32, shape, axis)


def ones_where(mask):
    return jnp.where(mask, 1.0, 0.0).astype(jnp.bfloat16)


def exact_dot(a, b):
    return jnp.dot(a, b, preferred_element_type=jnp.float32)


def kernel(
    sizes,
    hidden_hbm,
    grad_hbm,
    weight_hbm,
    moment_hbm,
    held_hbm,
    shift_hbm,
    out_ref,
    new_moment_ref,
    hidden,
    grad_ref,
    weight,
    moment,
    held_ref,
    shift_ref,
    stage,
    recv,
    mixed,
    spread,
    load_sem,
    grad_sem,
    table_sem,
    hub_sem,
    all_sem,
    send_sem,
    recv_sem,
    back_send_sem,
    back_recv_sem,
    far_recv_sem,
    spare,
    forward_send_sem,
    forward_recv_sem,
):
    size_x, size_y, size_z = sizes
    workers = size_x * size_y * size_z
    width = stage.shape[-1]
    groups, _, span = hidden.shape
    columns = stage.shape[1]
    parts = out_ref.shape[0] // TILE
    chunks = recv.shape[0]
    rounds = shift_ref.shape[0]
    my_x, my_y, my_z = lax.axis_index("gx"), lax.axis_index("gy"), lax.axis_index("gz")
    me = (my_x * size_y + my_y) * size_z + my_z
    slot = my_x + size_x * (my_y + size_y * my_z)

    plane = size_y * size_z
    half = workers // 2
    side = lax.div(me, half)
    lines = plane // GROUP
    layers = (half if columns == workers else columns) // plane
    my_line = lax.div(lax.rem(me, plane), GROUP)

    def ranked(step):
        far = 1 - lax.div(step, half)
        turn = (side ^ far) * (size_x - 1)
        layer = lax.div(lax.rem(step, half), plane) ^ turn
        return layer * plane + ((me & (plane - 1)) ^ (plane - 1 - lax.rem(step, plane)))

    def pair(group):
        side_groups = layers * lines
        order = lax.rem(group, side_groups)
        turn = my_line ^ ((lines - lax.div(order, layers)) & (lines - 1))
        layer = lax.rem(order, layers)
        if columns == workers:
            layer = layer ^ ((side ^ (1 - lax.div(group, side_groups))) * (size_x - 1))
        return layer * lines + turn

    def loads(group):
        place = pair(group)
        cut = pl.ds(pl.multiple_of(place * span, 128), span)
        return [
            pltpu.make_async_copy(source.at[:, cut], kept.at[place], load_sem.at[group])
            for source, kept in (
                (hidden_hbm, hidden),
                (moment_hbm, moment),
                (weight_hbm, weight),
            )
        ]

    def load(group, carry):
        for copy in loads(group):
            copy.start()
        return carry

    barrier = pltpu.get_barrier_semaphore()
    hub = my_x == 0

    def signal(sem, device):
        pl.semaphore_signal(sem, inc=1, device_id=device, device_id_type=LOGICAL)

    mates = size_x * GROUP - 1

    def greet(step, carry):
        mate = mates - step
        signal(barrier, me ^ (lax.div(mate, GROUP) * plane + lax.rem(mate, GROUP)))
        return carry

    def greet_hub(step, carry):
        signal(barrier, me ^ ((step + 1) * GROUP))
        return carry

    def tell_hub(step, carry):
        signal(hub_sem, me ^ ((step + 1) * GROUP))
        return carry

    def tell_line(step, carry):
        signal(all_sem, me + (step + 1) * plane)
        return carry

    grad_copy = pltpu.make_async_copy(grad_hbm, grad_ref, grad_sem.at[0])
    table_copies = [
        pltpu.make_async_copy(held_hbm, held_ref, table_sem.at[0]),
        pltpu.make_async_copy(shift_hbm, shift_ref, table_sem.at[1]),
    ]
    grad_copy.start()
    load(0, 0)
    lax.fori_loop(0, mates, greet, 0)

    @pl.when(hub)
    def _():
        lax.fori_loop(0, lines - 1, greet_hub, 0)
    lax.fori_loop(1, groups, load, 0)
    for copy in table_copies:
        copy.start()

    def place_of(part, where):
        block = part * columns
        return block // workers, block % workers + where

    def send(part, where):
        chunk, device = place_of(part, where)

        @pl.when(device != me)
        def _():
            pltpu.make_async_remote_copy(
                src_ref=stage.at[part, where],
                dst_ref=recv.at[chunk, slot],
                send_sem=send_sem.at[chunk],
                recv_sem=recv_sem.at[chunk],
                device_id=device,
                device_id_type=LOGICAL,
            ).start()

    early = [part for part in range(parts) if place_of(part, 0)[0] == 0]
    late = [part for part in range(parts) if place_of(part, 0)[0] > 0]

    def compute(group):
        place = pair(group)
        for copy in loads(group):
            copy.wait()
        grad = exact_dot(grad_ref[...], hidden[place])
        velocity = beta_keep * moment[place].astype(jnp.float32) + grad
        cut = pl.ds(pl.multiple_of(place * span, 128), span)
        new_moment_ref[:, cut] = velocity.astype(jnp.bfloat16)
        stepped = (weight[place].astype(jnp.float32) - learn_rate * velocity).astype(
            jnp.bfloat16
        )
        for k in range(GROUP):
            for part in range(parts):
                stage[part, place * GROUP + k] = stepped[
                    part * TILE : (part + 1) * TILE, k * width : (k + 1) * width
                ]

    def send_parts(which, group):
        for k in range(GROUP):
            for part in which:
                send(part, pair(group) * GROUP + k)

    def compute_ahead(group, carry):
        compute(group)
        return carry

    def send_ahead(group, carry):
        send_parts(early, group)
        return carry

    def compute_and_send(group, carry):
        compute(group)
        send_parts(early, group - 1)
        return carry

    def send_late(group, carry):
        send_parts(late, group)
        return carry

    grad_copy.wait()
    compute(jnp.int32(0))
    pl.semaphore_wait(barrier, mates + jnp.where(hub, lines - 1, 0))

    @pl.when(hub)
    def _():
        lax.fori_loop(0, lines - 1, tell_hub, 0)

    send_parts(early, jnp.int32(0))
    for group in range(1, layers):
        compute(jnp.int32(group))
        send_parts(early, jnp.int32(group))
    for group in range(layers):
        send_parts(late, jnp.int32(group))
    ahead = min(layers + 4, groups - 1)
    lax.fori_loop(layers, ahead, compute_ahead, 0)

    @pl.when(hub)
    def _():
        pl.semaphore_wait(hub_sem, lines - 1)
        lax.fori_loop(0, size_x - 1, tell_line, 0)

    @pl.when(jnp.logical_not(hub))
    def _():
        pl.semaphore_wait(all_sem, 1)

    lax.fori_loop(layers, ahead - 1, send_ahead, 0)
    lax.fori_loop(ahead, groups, compute_and_send, 0)
    send_parts(early, jnp.int32(groups - 1))
    if late:
        lax.fori_loop(layers, groups, send_late, 0)
    for chunk in range(chunks):
        block = chunk * workers + me
        recv[chunk, slot] = stage[lax.div(block, columns), lax.rem(block, columns)]
    for copy in table_copies:
        copy.wait()

    square = (workers, workers)
    gap = lax.rem(iota(square, 0) - iota(square, 1) + workers, workers)
    level = jnp.full(square, -1, jnp.int32)
    for power in range(workers.bit_length() - 1):
        level = jnp.where(gap == 1 << power, power, level)
    table = ones_where(held_ref[...] == iota(square, 0))
    for step in range(rounds):
        turn = ones_where((gap == 0) | (level == shift_ref[step]))
        table = exact_dot(turn, table).astype(jnp.bfloat16)
    distinct = workers // 2
    table = (table[:distinct].astype(jnp.float32) * 0.5**rounds).astype(jnp.bfloat16)
    wide = (workers, workers * TILE)
    table = exact_dot(table, ones_where(iota(wide, 1) // TILE == iota(wide, 0))).astype(
        jnp.bfloat16
    )
    height = min(256, distinct * TILE)

    def fill(step, carry):
        tall = (height, distinct)
        pick = ones_where((iota(tall, 0) + step * height) // TILE == iota(tall, 1))
        full = (height, workers * TILE)
        same = iota(full, 0) % TILE == iota(full, 1) % TILE
        spread[pl.ds(pl.multiple_of(step * height, height), height), :] = jnp.where(
            same, exact_dot(pick, table), 0.0
        ).astype(jnp.bfloat16)
        return carry

    lax.fori_loop(0, distinct * TILE // height, fill, 0)

    def pieces_wait(sem, count=workers - 1):
        ref = recv.at[0, pl.ds(0, count)]
        pltpu.make_async_copy(ref, ref, sem).wait()

    def mirror(device):
        return device ^ ((size_x - 1) * plane)

    def home(chunk, owner):
        block = chunk * workers + owner
        row = pl.multiple_of(lax.div(block, columns) * TILE, TILE)
        first = pl.multiple_of(lax.rem(block, columns) * width, 128)
        return pl.ds(row, TILE), pl.ds(first, width)

    mine = lax.rem(me, half)
    def forward_all(chunk):
        pieces_wait(far_recv_sem.at[chunk], half - 1)

        def forward(step, carry):
            owner = ranked(step)

            @pl.when(owner != mirror(me))
            def _():
                pltpu.make_async_remote_copy(
                    src_ref=out_ref.at[home(chunk, owner)],
                    dst_ref=spare.at[chunk, mine],
                    send_sem=forward_send_sem.at[chunk],
                    recv_sem=forward_recv_sem.at[chunk],
                    device_id=mirror(owner),
                    device_id_type=LOGICAL,
                ).start()

            return carry

        lax.fori_loop(0, half, forward, 0)
        spare[chunk, mine] = jnp.zeros((TILE, width), jnp.bfloat16)

    for chunk in range(chunks):
        pieces_wait(recv_sem.at[chunk])
        got = recv[chunk].reshape(workers * TILE, width)

        def blend(step, carry):
            result = exact_dot(
                spread[pl.ds(pl.multiple_of(step * height, height), height), :], got
            )
            mixed[chunk, pl.ds(step * (height // TILE), height // TILE)] = result.astype(
                jnp.bfloat16
            ).reshape(height // TILE, TILE, width)
            return carry

        lax.fori_loop(0, distinct * TILE // height, blend, 0)
        out_ref[home(chunk, me)] = mixed[chunk, mine]

        def back(step, absent, sem):
            device = ranked(step)

            @pl.when(device != absent)
            def _():
                pltpu.make_async_remote_copy(
                    src_ref=mixed.at[chunk, lax.rem(device, half)],
                    dst_ref=out_ref.at[home(chunk, me)],
                    send_sem=back_send_sem.at[chunk],
                    recv_sem=sem.at[chunk],
                    device_id=device,
                    device_id_type=LOGICAL,
                ).start()

        def back_far(step, carry):
            last = chunk == chunks - 1
            back(step, me if last else mirror(me), back_recv_sem if last else far_recv_sem)
            return carry

        def back_near(step, carry):
            back(step, me, back_recv_sem)
            return carry

        if chunk == chunks - 1:
            lax.fori_loop(half, workers, back_near, 0)
            lax.fori_loop(0, half // 2, back_far, 0)
            for earlier in range(chunks - 1):
                forward_all(earlier)
            lax.fori_loop(half // 2, half, back_far, 0)
        else:
            lax.fori_loop(0, half, back_far, 0)
            lax.fori_loop(half, workers, back_near, 0)

    for chunk in range(chunks - 1):
        pieces_wait(forward_recv_sem.at[chunk], half - 1)
        total = jnp.zeros((TILE, width), jnp.float32)
        for k in range(half):
            piece = spare[chunk, k].astype(jnp.float32)
            total = total - piece if k % 2 else total + piece
        total = jnp.where(lax.rem(me, 2) == 1, total, -total)
        out_ref[home(chunk, mirror(me))] = total.astype(jnp.bfloat16)

    for chunk in range(chunks):
        last = chunk == chunks - 1
        pieces_wait(send_sem.at[chunk])
        pieces_wait(back_send_sem.at[chunk], workers - 1 if last else workers - 2)
        if not last:
            pieces_wait(forward_send_sem.at[chunk], half - 1)
        pieces_wait(back_recv_sem.at[chunk], workers - 1 if last else half - 1)


def store(mixed_ref, moment_ref, mixed_hbm, moment_hbm, sem):
    copies = [
        pltpu.make_async_copy(mixed_ref, mixed_hbm, sem.at[0]),
        pltpu.make_async_copy(moment_ref, moment_hbm, sem.at[1]),
    ]
    for copy in copies:
        copy.start()
    for copy in copies:
        copy.wait()


def shards(sizes, hidden_acts, output_grad, weights, momentum, worker_of_slot, round_shift):
    hidden = hidden_acts.reshape(hidden_acts.shape[-2:])
    grad_out = output_grad.reshape(output_grad.shape[-2:]).T
    weight = weights.reshape(weights.shape[-2:])
    moment = momentum.reshape(momentum.shape[-2:])
    workers = sizes[0] * sizes[1] * sizes[2]
    tokens, features = hidden.shape
    rows = weight.shape[0]
    parts = rows // TILE
    width = max(128, features // workers)
    columns = features // width
    chunks = parts * columns // workers
    distinct = workers // 2
    groups = columns // GROUP
    anywhere = pl.BlockSpec(memory_space=pl.ANY)
    vmem = pl.BlockSpec(memory_space=pltpu.VMEM)
    half = jnp.bfloat16
    mixed, new_moment = pl.pallas_call(
        functools.partial(kernel, sizes),
        out_shape=[pltpu.VMEM((rows, features), half)] * 2,
        in_specs=[anywhere] * 6,
        out_specs=[vmem, vmem],
        scratch_shapes=[
            pltpu.VMEM((groups, tokens, GROUP * width), half),
            pltpu.VMEM((rows, tokens), half),
            pltpu.VMEM((groups, rows, GROUP * width), half),
            pltpu.VMEM((groups, rows, GROUP * width), half),
            pltpu.VMEM((1, workers), jnp.int32),
            pltpu.SMEM(round_shift.shape, jnp.int32),
            pltpu.VMEM((parts, columns, TILE, width), half),
            pltpu.VMEM((chunks, workers, TILE, width), half),
            pltpu.VMEM((chunks, distinct, TILE, width), half),
            pltpu.VMEM((distinct * TILE, workers * TILE), half),
            pltpu.SemaphoreType.DMA((groups,)),
            pltpu.SemaphoreType.DMA((1,)),
            pltpu.SemaphoreType.DMA((2,)),
            pltpu.SemaphoreType.REGULAR,
            pltpu.SemaphoreType.REGULAR,
            pltpu.SemaphoreType.DMA((chunks,)),
            pltpu.SemaphoreType.DMA((chunks,)),
            pltpu.SemaphoreType.DMA((chunks,)),
            pltpu.SemaphoreType.DMA((chunks,)),
            pltpu.SemaphoreType.DMA((chunks,)),
            pltpu.VMEM((max(1, chunks - 1), distinct, TILE, width), half),
            pltpu.SemaphoreType.DMA((chunks,)),
            pltpu.SemaphoreType.DMA((chunks,)),
        ],
        compiler_params=pltpu.CompilerParams(
            collective_id=0, has_side_effects=True, vmem_limit_bytes=60 * 1024 * 1024
        ),
        name="step_and_gossip",
    )(hidden, grad_out, weight, moment, worker_of_slot.reshape(1, workers), round_shift)
    mixed, new_moment = pl.pallas_call(
        store,
        out_shape=[jax.ShapeDtypeStruct((rows, features), half)] * 2,
        in_specs=[anywhere, anywhere],
        out_specs=[anywhere, anywhere],
        scratch_shapes=[pltpu.SemaphoreType.DMA((2,))],
        name="store",
    )(
        pltpu.with_memory_space_constraint(mixed, pltpu.VMEM),
        pltpu.with_memory_space_constraint(new_moment, pltpu.VMEM),
    )
    return (mixed.reshape(weights.shape), new_moment.reshape(momentum.shape))


def solution(mesh):
    sizes = (mesh.shape["gx"], mesh.shape["gy"], mesh.shape["gz"])
    placed = (
        P("gz", "gy", "gx", None, None),
        P("gz", "gy", "gx", None, None),
        P("gz", "gy", "gx", None, None),
        P("gz", "gy", "gx", None, None),
        P(),
        P(),
    )
    return jax.shard_map(
        functools.partial(shards, sizes),
        mesh=mesh,
        in_specs=placed,
        out_specs=(P("gx", "gy", "gz", None, None), P("gz", "gy", "gx", None, None)),
        check_vma=False,
    )
```

```python
import functools

import jax
import jax.numpy as jnp
from jax import lax
from jax.experimental import pallas as pl
from jax.experimental.pallas import tpu as pltpu
from jax.sharding import PartitionSpec as P

learn_rate = 0.01
beta_keep = 0.9
TILE = 16
GROUP = 2
LOGICAL = pl.DeviceIdType.LOGICAL


def iota(shape, axis):
    return lax.broadcasted_iota(jnp.int32, shape, axis)


def ones_where(mask):
    return jnp.where(mask, 1.0, 0.0).astype(jnp.bfloat16)


def exact_dot(a, b):
    return jnp.dot(a, b, preferred_element_type=jnp.float32)


def kernel(
    sizes,
    hidden_hbm,
    grad_hbm,
    weight_hbm,
    moment_hbm,
    held_hbm,
    shift_hbm,
    out_ref,
    new_moment_ref,
    hidden,
    grad_ref,
    weight,
    moment,
    held_ref,
    shift_ref,
    stage,
    recv,
    mixed,
    spread,
    load_sem,
    grad_sem,
    table_sem,
    line_sem,
    hub_sem,
    all_sem,
    send_sem,
    recv_sem,
    back_send_sem,
    back_recv_sem,
    far_recv_sem,
    spare,
    forward_send_sem,
    forward_recv_sem,
):
    size_x, size_y, size_z = sizes
    workers = size_x * size_y * size_z
    width = stage.shape[-1]
    groups, _, span = hidden.shape
    columns = stage.shape[1]
    parts = out_ref.shape[0] // TILE
    chunks = recv.shape[0]
    rounds = shift_ref.shape[0]
    my_x, my_y, my_z = lax.axis_index("gx"), lax.axis_index("gy"), lax.axis_index("gz")
    me = (my_x * size_y + my_y) * size_z + my_z
    slot = my_x + size_x * (my_y + size_y * my_z)

    plane = size_y * size_z
    half = workers // 2
    side = lax.div(me, half)
    lines = plane // GROUP
    layers = (half if columns == workers else columns) // plane
    my_line = lax.div(lax.rem(me, plane), GROUP)

    def ranked(step):
        far = 1 - lax.div(step, half)
        turn = (side ^ far) * (size_x - 1)
        layer = lax.div(lax.rem(step, half), plane) ^ turn
        return layer * plane + ((me & (plane - 1)) ^ (plane - 1 - lax.rem(step, plane)))

    def pair(group):
        side_groups = layers * lines
        order = lax.rem(group, side_groups)
        turn = my_line ^ ((lines - lax.div(order, layers)) & (lines - 1))
        layer = lax.rem(order, layers)
        if columns == workers:
            far = 1 - lax.div(group, side_groups)
            layer = layer ^ my_x ^ (far * (size_x - 1))
        return layer * lines + turn

    def loads(group):
        place = pair(group)
        cut = pl.ds(pl.multiple_of(place * span, 128), span)
        return [
            pltpu.make_async_copy(source.at[:, cut], kept.at[place], load_sem.at[group])
            for source, kept in (
                (hidden_hbm, hidden),
                (moment_hbm, moment),
                (weight_hbm, weight),
            )
        ]

    def load(group, carry):
        for copy in loads(group):
            copy.start()
        return carry

    barrier = pltpu.get_barrier_semaphore()
    hub = my_x == 0

    def signal(sem, device):
        pl.semaphore_signal(sem, inc=1, device_id=device, device_id_type=LOGICAL)

    def mirror(device):
        return device ^ ((size_x - 1) * plane)

    half_x = size_x // 2
    lead_x = side * (size_x - 1)
    right_lead = my_x == size_x - 1
    leader = jnp.logical_or(hub, right_lead)
    left_inner = jnp.logical_and(my_x > 0, my_x < half_x)
    right_inner = jnp.logical_and(my_x >= half_x, my_x < size_x - 1)
    lead = me ^ ((my_x ^ lead_x) * plane)

    def greet_side(step, carry):
        signal(barrier, me ^ ((step + 1) * plane))
        signal(barrier, me ^ ((step + 1) * plane) ^ 1)
        return carry

    def tell_side(step, carry):
        signal(line_sem, me ^ ((step + 1) * plane))
        return carry

    def greet():
        signal(barrier, mirror(me))
        signal(barrier, mirror(me) ^ 1)
        signal(barrier, me ^ 1)

        @pl.when(jnp.logical_not(leader))
        def _():
            signal(barrier, lead)
            signal(barrier, lead ^ 1)

        @pl.when(hub)
        def _():
            lax.fori_loop(0, half_x - 1, greet_side, 0)
            lax.fori_loop(0, lines - 1, greet_hub, 0)

    others = 2 * (half_x - 1)
    expected = 3 + jnp.where(leader, others, 0) + jnp.where(left_inner, 2, 0)
    expected = expected + jnp.where(hub, lines - 1, 0)

    def greet_hub(step, carry):
        signal(barrier, me ^ ((step + 1) * GROUP))
        return carry

    def tell_hub(step, carry):
        signal(hub_sem, me ^ ((step + 1) * GROUP))
        return carry

    def tell_line(step, carry):
        signal(all_sem, me ^ ((step + 1) * plane))
        return carry

    grad_copy = pltpu.make_async_copy(grad_hbm, grad_ref, grad_sem.at[0])
    table_copies = [
        pltpu.make_async_copy(held_hbm, held_ref, table_sem.at[0]),
        pltpu.make_async_copy(shift_hbm, shift_ref, table_sem.at[1]),
    ]
    grad_copy.start()
    load(0, 0)
    greet()
    lax.fori_loop(1, groups, load, 0)
    for copy in table_copies:
        copy.start()

    def place_of(part, where):
        block = part * columns
        return block // workers, block % workers + where

    def send(part, where):
        chunk, device = place_of(part, where)

        @pl.when(device != me)
        def _():
            pltpu.make_async_remote_copy(
                src_ref=stage.at[part, where],
                dst_ref=recv.at[chunk, slot],
                send_sem=send_sem.at[chunk],
                recv_sem=recv_sem.at[chunk],
                device_id=device,
                device_id_type=LOGICAL,
            ).start()

    early = [part for part in range(parts) if place_of(part, 0)[0] == 0]
    late = [part for part in range(parts) if place_of(part, 0)[0] > 0]

    def compute(group):
        place = pair(group)
        for copy in loads(group):
            copy.wait()
        grad = exact_dot(grad_ref[...], hidden[place])
        velocity = beta_keep * moment[place].astype(jnp.float32) + grad
        cut = pl.ds(pl.multiple_of(place * span, 128), span)
        new_moment_ref[:, cut] = velocity.astype(jnp.bfloat16)
        stepped = (weight[place].astype(jnp.float32) - learn_rate * velocity).astype(
            jnp.bfloat16
        )
        for k in range(GROUP):
            for part in range(parts):
                stage[part, place * GROUP + k] = stepped[
                    part * TILE : (part + 1) * TILE, k * width : (k + 1) * width
                ]

    def send_parts(which, group):
        for k in range(GROUP):
            for part in which:
                send(part, pair(group) * GROUP + k)

    def compute_ahead(group, carry):
        compute(group)
        return carry

    def send_ahead(group, carry):
        send_parts(early, group)
        return carry

    def compute_and_send(group, carry):
        compute(group)
        send_parts(early, group - 1)
        return carry

    def send_late(group, carry):
        send_parts(late, group)
        return carry

    grad_copy.wait()
    compute(jnp.int32(0))
    pl.semaphore_wait(barrier, expected)

    @pl.when(left_inner)
    def _():
        signal(line_sem, lead)

    @pl.when(hub)
    def _():
        pl.semaphore_wait(line_sem, half_x - 1)

    @pl.when(leader)
    def _():
        lax.fori_loop(0, half_x - 1, tell_side, 0)

    @pl.when(hub)
    def _():
        lax.fori_loop(0, lines - 1, tell_hub, 0)

    def send_all(group):
        send_parts(early, jnp.int32(group))
        send_parts(late, jnp.int32(group))

    if columns == workers:
        send_all(0)
    compute(jnp.int32(1))

    @pl.when(jnp.logical_not(leader))
    def _():
        pl.semaphore_wait(line_sem, 1)

    @pl.when(right_inner)
    def _():
        signal(line_sem, lead)

    @pl.when(right_lead)
    def _():
        pl.semaphore_wait(line_sem, half_x - 1)

    if half_x > 2:

        @pl.when(right_lead)
        def _():
            lax.fori_loop(0, half_x - 1, tell_side, 0)

        @pl.when(right_inner)
        def _():
            pl.semaphore_wait(line_sem, 1)

    if columns != workers:
        send_all(0)
    send_all(1)
    for group in range(2, layers):
        compute(jnp.int32(group))
        send_all(group)
    ahead = min(layers + 4, groups - 1)
    lax.fori_loop(layers, ahead, compute_ahead, 0)

    @pl.when(hub)
    def _():
        pl.semaphore_wait(hub_sem, lines - 1)
        lax.fori_loop(0, size_x - 1, tell_line, 0)

    @pl.when(jnp.logical_not(hub))
    def _():
        pl.semaphore_wait(all_sem, 1)

    lax.fori_loop(layers, ahead - 1, send_ahead, 0)
    lax.fori_loop(ahead, groups, compute_and_send, 0)
    send_parts(early, jnp.int32(groups - 1))
    if late:
        lax.fori_loop(layers, groups, send_late, 0)
    for chunk in range(chunks):
        block = chunk * workers + me
        recv[chunk, slot] = stage[lax.div(block, columns), lax.rem(block, columns)]
    for copy in table_copies:
        copy.wait()

    square = (workers, workers)
    gap = lax.rem(iota(square, 0) - iota(square, 1) + workers, workers)
    level = jnp.full(square, -1, jnp.int32)
    for power in range(workers.bit_length() - 1):
        level = jnp.where(gap == 1 << power, power, level)
    table = ones_where(held_ref[...] == iota(square, 0))
    for step in range(rounds):
        turn = ones_where((gap == 0) | (level == shift_ref[step]))
        table = exact_dot(turn, table).astype(jnp.bfloat16)
    distinct = workers // 2
    table = (table[:distinct].astype(jnp.float32) * 0.5**rounds).astype(jnp.bfloat16)
    wide = (workers, workers * TILE)
    table = exact_dot(table, ones_where(iota(wide, 1) // TILE == iota(wide, 0))).astype(
        jnp.bfloat16
    )
    height = min(256, distinct * TILE)

    def fill(step, carry):
        tall = (height, distinct)
        pick = ones_where((iota(tall, 0) + step * height) // TILE == iota(tall, 1))
        full = (height, workers * TILE)
        same = iota(full, 0) % TILE == iota(full, 1) % TILE
        spread[pl.ds(pl.multiple_of(step * height, height), height), :] = jnp.where(
            same, exact_dot(pick, table), 0.0
        ).astype(jnp.bfloat16)
        return carry

    lax.fori_loop(0, distinct * TILE // height, fill, 0)

    def pieces_wait(sem, count=workers - 1):
        ref = recv.at[0, pl.ds(0, count)]
        pltpu.make_async_copy(ref, ref, sem).wait()

    def home(chunk, owner):
        block = chunk * workers + owner
        row = pl.multiple_of(lax.div(block, columns) * TILE, TILE)
        first = pl.multiple_of(lax.rem(block, columns) * width, 128)
        return pl.ds(row, TILE), pl.ds(first, width)

    mine = lax.rem(me, half)
    def forward_all(chunk):
        pieces_wait(far_recv_sem.at[chunk], half - 1)

        def forward(step, carry):
            owner = ranked(step)

            @pl.when(owner != mirror(me))
            def _():
                pltpu.make_async_remote_copy(
                    src_ref=out_ref.at[home(chunk, owner)],
                    dst_ref=spare.at[chunk, mine],
                    send_sem=forward_send_sem.at[chunk],
                    recv_sem=forward_recv_sem.at[chunk],
                    device_id=mirror(owner),
                    device_id_type=LOGICAL,
                ).start()

            return carry

        lax.fori_loop(0, half, forward, 0)
        spare[chunk, mine] = jnp.zeros((TILE, width), jnp.bfloat16)

    for chunk in range(chunks):
        pieces_wait(recv_sem.at[chunk])
        got = recv[chunk].reshape(workers * TILE, width)

        def blend(step, carry):
            result = exact_dot(
                spread[pl.ds(pl.multiple_of(step * height, height), height), :], got
            )
            mixed[chunk, pl.ds(step * (height // TILE), height // TILE)] = result.astype(
                jnp.bfloat16
            ).reshape(height // TILE, TILE, width)
            return carry

        lax.fori_loop(0, distinct * TILE // height, blend, 0)
        out_ref[home(chunk, me)] = mixed[chunk, mine]

        def back(step, absent, sem):
            device = ranked(step)

            @pl.when(device != absent)
            def _():
                pltpu.make_async_remote_copy(
                    src_ref=mixed.at[chunk, lax.rem(device, half)],
                    dst_ref=out_ref.at[home(chunk, me)],
                    send_sem=back_send_sem.at[chunk],
                    recv_sem=sem.at[chunk],
                    device_id=device,
                    device_id_type=LOGICAL,
                ).start()

        def back_far(step, carry):
            last = chunk == chunks - 1
            back(step, me if last else mirror(me), back_recv_sem if last else far_recv_sem)
            return carry

        def back_near(step, carry):
            back(step, me, back_recv_sem)
            return carry

        if chunk == chunks - 1:
            lax.fori_loop(half, workers, back_near, 0)
            lax.fori_loop(0, half // 2, back_far, 0)
            for earlier in range(chunks - 1):
                forward_all(earlier)
            lax.fori_loop(half // 2, half, back_far, 0)
        else:
            lax.fori_loop(0, half, back_far, 0)
            lax.fori_loop(half, workers, back_near, 0)

    for chunk in range(chunks - 1):
        pieces_wait(forward_recv_sem.at[chunk], half - 1)
        total = jnp.zeros((TILE, width), jnp.float32)
        for k in range(half):
            piece = spare[chunk, k].astype(jnp.float32)
            total = total - piece if k % 2 else total + piece
        total = jnp.where(lax.rem(me, 2) == 1, total, -total)
        out_ref[home(chunk, mirror(me))] = total.astype(jnp.bfloat16)

    for chunk in range(chunks):
        last = chunk == chunks - 1
        pieces_wait(send_sem.at[chunk])
        pieces_wait(back_send_sem.at[chunk], workers - 1 if last else workers - 2)
        if not last:
            pieces_wait(forward_send_sem.at[chunk], half - 1)
        pieces_wait(back_recv_sem.at[chunk], workers - 1 if last else half - 1)


def store(mixed_ref, moment_ref, mixed_hbm, moment_hbm, sem):
    copies = [
        pltpu.make_async_copy(mixed_ref, mixed_hbm, sem.at[0]),
        pltpu.make_async_copy(moment_ref, moment_hbm, sem.at[1]),
    ]
    for copy in copies:
        copy.start()
    for copy in copies:
        copy.wait()


def shards(sizes, hidden_acts, output_grad, weights, momentum, worker_of_slot, round_shift):
    hidden = hidden_acts.reshape(hidden_acts.shape[-2:])
    grad_out = output_grad.reshape(output_grad.shape[-2:]).T
    weight = weights.reshape(weights.shape[-2:])
    moment = momentum.reshape(momentum.shape[-2:])
    workers = sizes[0] * sizes[1] * sizes[2]
    tokens, features = hidden.shape
    rows = weight.shape[0]
    parts = rows // TILE
    width = max(128, features // workers)
    columns = features // width
    chunks = parts * columns // workers
    distinct = workers // 2
    groups = columns // GROUP
    anywhere = pl.BlockSpec(memory_space=pl.ANY)
    vmem = pl.BlockSpec(memory_space=pltpu.VMEM)
    half = jnp.bfloat16
    mixed, new_moment = pl.pallas_call(
        functools.partial(kernel, sizes),
        out_shape=[pltpu.VMEM((rows, features), half)] * 2,
        in_specs=[anywhere] * 6,
        out_specs=[vmem, vmem],
        scratch_shapes=[
            pltpu.VMEM((groups, tokens, GROUP * width), half),
            pltpu.VMEM((rows, tokens), half),
            pltpu.VMEM((groups, rows, GROUP * width), half),
            pltpu.VMEM((groups, rows, GROUP * width), half),
            pltpu.VMEM((1, workers), jnp.int32),
            pltpu.SMEM(round_shift.shape, jnp.int32),
            pltpu.VMEM((parts, columns, TILE, width), half),
            pltpu.VMEM((chunks, workers, TILE, width), half),
            pltpu.VMEM((chunks, distinct, TILE, width), half),
            pltpu.VMEM((distinct * TILE, workers * TILE), half),
            pltpu.SemaphoreType.DMA((groups,)),
            pltpu.SemaphoreType.DMA((1,)),
            pltpu.SemaphoreType.DMA((2,)),
            pltpu.SemaphoreType.REGULAR,
            pltpu.SemaphoreType.REGULAR,
            pltpu.SemaphoreType.REGULAR,
            pltpu.SemaphoreType.DMA((chunks,)),
            pltpu.SemaphoreType.DMA((chunks,)),
            pltpu.SemaphoreType.DMA((chunks,)),
            pltpu.SemaphoreType.DMA((chunks,)),
            pltpu.SemaphoreType.DMA((chunks,)),
            pltpu.VMEM((max(1, chunks - 1), distinct, TILE, width), half),
            pltpu.SemaphoreType.DMA((chunks,)),
            pltpu.SemaphoreType.DMA((chunks,)),
        ],
        compiler_params=pltpu.CompilerParams(
            collective_id=0, has_side_effects=True, vmem_limit_bytes=60 * 1024 * 1024
        ),
        name="step_and_gossip",
    )(hidden, grad_out, weight, moment, worker_of_slot.reshape(1, workers), round_shift)
    mixed, new_moment = pl.pallas_call(
        store,
        out_shape=[jax.ShapeDtypeStruct((rows, features), half)] * 2,
        in_specs=[anywhere, anywhere],
        out_specs=[anywhere, anywhere],
        scratch_shapes=[pltpu.SemaphoreType.DMA((2,))],
        name="store",
    )(
        pltpu.with_memory_space_constraint(mixed, pltpu.VMEM),
        pltpu.with_memory_space_constraint(new_moment, pltpu.VMEM),
    )
    return (mixed.reshape(weights.shape), new_moment.reshape(momentum.shape))


def solution(mesh):
    sizes = (mesh.shape["gx"], mesh.shape["gy"], mesh.shape["gz"])
    placed = (
        P("gz", "gy", "gx", None, None),
        P("gz", "gy", "gx", None, None),
        P("gz", "gy", "gx", None, None),
        P("gz", "gy", "gx", None, None),
        P(),
        P(),
    )
    return jax.shard_map(
        functools.partial(shards, sizes),
        mesh=mesh,
        in_specs=placed,
        out_specs=(P("gx", "gy", "gz", None, None), P("gz", "gy", "gx", None, None)),
        check_vma=False,
    )
```

```python
import functools

import jax
import jax.numpy as jnp
from jax import lax
from jax.experimental import pallas as pl
from jax.experimental.pallas import tpu as pltpu
from jax.sharding import PartitionSpec as P

learn_rate = 0.01
beta_keep = 0.9
TILE = 16
GROUP = 2
BANK = 4
LOGICAL = pl.DeviceIdType.LOGICAL


def iota(shape, axis):
    return lax.broadcasted_iota(jnp.int32, shape, axis)


def ones_where(mask):
    return jnp.where(mask, 1.0, 0.0).astype(jnp.bfloat16)


def exact_dot(a, b):
    return jnp.dot(a, b, preferred_element_type=jnp.float32)


def kernel(
    sizes,
    hidden_hbm,
    grad_hbm,
    weight_hbm,
    moment_hbm,
    held_hbm,
    shift_hbm,
    out_ref,
    new_moment_ref,
    hidden,
    grad_ref,
    weight,
    moment,
    held_ref,
    shift_ref,
    stage,
    recv,
    mixed,
    spread,
    load_sem,
    table_sem,
    line_sem,
    hub_sem,
    all_sem,
    sent_sem,
    recv_sem,
    back_recv_sem,
    far_recv_sem,
    forward_recv_sem,
    spare,
):
    size_x, size_y, size_z = sizes
    workers = size_x * size_y * size_z
    width = stage.shape[-1]
    groups, _, span = hidden.shape
    columns = stage.shape[1]
    parts = out_ref.shape[0] // TILE
    chunks = recv.shape[0]
    rounds = shift_ref.shape[0]
    my_x, my_y, my_z = lax.axis_index("gx"), lax.axis_index("gy"), lax.axis_index("gz")
    me = (my_x * size_y + my_y) * size_z + my_z
    slot = my_x + size_x * (my_y + size_y * my_z)

    plane = size_y * size_z
    half = workers // 2
    side = lax.div(me, half)
    lines = plane // GROUP
    layers = (half if columns == workers else columns) // plane
    my_line = lax.div(lax.rem(me, plane), GROUP)

    def ranked(step):
        far = 1 - lax.div(step, half)
        turn = (side ^ far) * (size_x - 1)
        layer = lax.div(lax.rem(step, half), plane) ^ turn
        return layer * plane + ((me & (plane - 1)) ^ (plane - 1 - lax.rem(step, plane)))

    def pair(group):
        side_groups = layers * lines
        order = lax.rem(group, side_groups)
        turn = my_line ^ ((lines - lax.div(order, layers)) & (lines - 1))
        layer = lax.rem(order, layers)
        if columns == workers:
            far = 1 - lax.div(group, side_groups)
            layer = layer ^ my_x ^ (far * (size_x - 1))
        return layer * lines + turn

    def bank(group):
        return GROUP + lax.div(group + BANK - 2, BANK)

    def loads(group, first=0, count=GROUP, sem=None):
        place = pair(group)
        take = count * width
        cut = pl.ds(pl.multiple_of(place * span + first * width, 128), take)
        return [
            pltpu.make_async_copy(
                source.at[:, cut],
                kept.at[place, :, pl.ds(first * width, take)],
                load_sem.at[bank(group) if sem is None else sem],
            )
            for source, kept in (
                (hidden_hbm, hidden),
                (moment_hbm, moment),
                (weight_hbm, weight),
            )
        ]

    def load(group, carry):
        for copy in loads(group):
            copy.start()
        return carry

    def single(k):
        return loads(0, k, 1, k)

    barrier = pltpu.get_barrier_semaphore()
    hub = my_x == 0

    def signal(sem, device):
        pl.semaphore_signal(sem, inc=1, device_id=device, device_id_type=LOGICAL)

    def mirror(device):
        return device ^ ((size_x - 1) * plane)

    half_x = size_x // 2
    lead_x = side * (size_x - 1)
    right_lead = my_x == size_x - 1
    leader = jnp.logical_or(hub, right_lead)
    left_inner = jnp.logical_and(my_x > 0, my_x < half_x)
    right_inner = jnp.logical_and(my_x >= half_x, my_x < size_x - 1)
    lead = me ^ ((my_x ^ lead_x) * plane)

    def greet_side(step, carry):
        signal(barrier, me ^ ((step + 1) * plane))
        signal(barrier, me ^ ((step + 1) * plane) ^ 1)
        return carry

    def tell_side(step, carry):
        signal(line_sem, me ^ ((step + 1) * plane))
        return carry

    def greet():
        signal(barrier, mirror(me))
        signal(barrier, mirror(me) ^ 1)
        signal(barrier, me ^ 1)

        @pl.when(jnp.logical_not(leader))
        def _():
            signal(barrier, lead)
            signal(barrier, lead ^ 1)

        @pl.when(hub)
        def _():
            lax.fori_loop(0, half_x - 1, greet_side, 0)
            lax.fori_loop(0, lines - 1, greet_hub, 0)

    others = 2 * (half_x - 1)
    expected = 3 + jnp.where(leader, others, 0) + jnp.where(left_inner, 2, 0)
    expected = expected + jnp.where(hub, lines - 1, 0)

    def greet_hub(step, carry):
        signal(barrier, me ^ ((step + 1) * GROUP))
        return carry

    def tell_hub(step, carry):
        signal(hub_sem, me ^ ((step + 1) * GROUP))
        return carry

    def tell_line(step, carry):
        signal(all_sem, me ^ ((step + 1) * plane))
        return carry

    grad_copy = pltpu.make_async_copy(grad_hbm, grad_ref, load_sem.at[0])
    table_copies = [
        pltpu.make_async_copy(held_hbm, held_ref, table_sem.at[0]),
        pltpu.make_async_copy(shift_hbm, shift_ref, table_sem.at[0]),
    ]
    grad_copy.start()
    for copy in single(0):
        copy.start()
    greet()
    for k in range(1, GROUP):
        for copy in single(k):
            copy.start()
    lax.fori_loop(1, groups, load, 0)
    for copy in table_copies:
        copy.start()

    def place_of(part, where):
        block = part * columns
        return block // workers, block % workers + where

    def send(part, where):
        chunk, device = place_of(part, where)

        @pl.when(device != me)
        def _():
            pltpu.make_async_remote_copy(
                src_ref=stage.at[part, where],
                dst_ref=recv.at[chunk, slot],
                send_sem=sent_sem.at[0],
                recv_sem=recv_sem.at[chunk],
                device_id=device,
                device_id_type=LOGICAL,
            ).start()

    early = [part for part in range(parts) if place_of(part, 0)[0] == 0]
    late = [part for part in range(parts) if place_of(part, 0)[0] > 0]

    def advance(place, first, count):
        low, take = first * width, count * width
        kept = (place, slice(None), slice(low, low + take))
        velocity = beta_keep * moment[kept].astype(jnp.float32) + exact_dot(
            grad_ref[...], hidden[kept]
        )
        cut = pl.ds(pl.multiple_of(place * span + low, 128), take)
        new_moment_ref[:, cut] = velocity.astype(jnp.bfloat16)
        stepped = (weight[kept].astype(jnp.float32) - learn_rate * velocity).astype(
            jnp.bfloat16
        )
        for k in range(count):
            for part in range(parts):
                stage[part, place * GROUP + first + k] = stepped[
                    part * TILE : (part + 1) * TILE, k * width : (k + 1) * width
                ]

    def compute(group):
        @pl.when((group < 2) | (lax.rem(group + BANK - 2, BANK) == 0))
        def _():
            for step in range(BANK):

                @pl.when((bank(group + step) == bank(group)) & (group + step < groups))
                def _():
                    for copy in loads(group + step):
                        copy.wait()

        advance(pair(group), 0, GROUP)

    def compute_single(k):
        for copy in single(k):
            copy.wait()
        advance(pair(0), k, 1)

    def send_parts(which, group):
        for k in range(GROUP):
            for part in which:
                send(part, pair(group) * GROUP + k)

    def compute_ahead(group, carry):
        compute(group)
        return carry

    def send_ahead(group, carry):
        send_parts(early, group)
        return carry

    def compute_and_send(group, carry):
        compute(group)
        send_parts(early, group - 1)
        return carry

    def send_late(group, carry):
        send_parts(late, group)
        return carry

    grad_copy.wait()
    compute_single(0)
    pl.semaphore_wait(barrier, expected)

    @pl.when(left_inner)
    def _():
        signal(line_sem, lead)

    @pl.when(hub)
    def _():
        pl.semaphore_wait(line_sem, half_x - 1)

    @pl.when(leader)
    def _():
        lax.fori_loop(0, half_x - 1, tell_side, 0)

    @pl.when(hub)
    def _():
        lax.fori_loop(0, lines - 1, tell_hub, 0)

    def send_all(group):
        send_parts(early, jnp.int32(group))
        send_parts(late, jnp.int32(group))

    for k in range(GROUP):
        if k:
            compute_single(k)
        if columns == workers:
            for part in range(parts):
                send(part, pair(0) * GROUP + k)
    compute(jnp.int32(1))

    @pl.when(jnp.logical_not(leader))
    def _():
        pl.semaphore_wait(line_sem, 1)

    @pl.when(right_inner)
    def _():
        signal(line_sem, lead)

    @pl.when(right_lead)
    def _():
        pl.semaphore_wait(line_sem, half_x - 1)

    if half_x > 2:

        @pl.when(right_lead)
        def _():
            lax.fori_loop(0, half_x - 1, tell_side, 0)

        @pl.when(right_inner)
        def _():
            pl.semaphore_wait(line_sem, 1)

    if columns != workers:
        send_all(0)
    send_all(1)
    for group in range(2, layers):
        compute(jnp.int32(group))
        send_all(group)
    ahead = min(layers + 4, groups - 1)
    lax.fori_loop(layers, ahead, compute_ahead, 0)

    @pl.when(hub)
    def _():
        pl.semaphore_wait(hub_sem, lines - 1)
        lax.fori_loop(0, size_x - 1, tell_line, 0)

    @pl.when(jnp.logical_not(hub))
    def _():
        pl.semaphore_wait(all_sem, 1)

    lax.fori_loop(layers, ahead - 1, send_ahead, 0)
    lax.fori_loop(ahead, groups, compute_and_send, 0)
    send_parts(early, jnp.int32(groups - 1))
    if late:
        lax.fori_loop(layers, groups, send_late, 0)
    for chunk in range(chunks):
        block = chunk * workers + me
        recv[chunk, slot] = stage[lax.div(block, columns), lax.rem(block, columns)]
    for copy in table_copies:
        copy.wait()

    square = (workers, workers)
    gap = lax.rem(iota(square, 0) - iota(square, 1) + workers, workers)
    level = jnp.full(square, -1, jnp.int32)
    for power in range(workers.bit_length() - 1):
        level = jnp.where(gap == 1 << power, power, level)
    table = ones_where(held_ref[...] == iota(square, 0))
    for step in range(rounds):
        turn = ones_where((gap == 0) | (level == shift_ref[step]))
        table = exact_dot(turn, table).astype(jnp.bfloat16)
    distinct = workers // 2
    table = (table[:distinct].astype(jnp.float32) * 0.5**rounds).astype(jnp.bfloat16)
    wide = (workers, workers * TILE)
    table = exact_dot(table, ones_where(iota(wide, 1) // TILE == iota(wide, 0))).astype(
        jnp.bfloat16
    )
    height = min(256, distinct * TILE)

    def fill(step, carry):
        tall = (height, distinct)
        pick = ones_where((iota(tall, 0) + step * height) // TILE == iota(tall, 1))
        full = (height, workers * TILE)
        same = iota(full, 0) % TILE == iota(full, 1) % TILE
        spread[pl.ds(pl.multiple_of(step * height, height), height), :] = jnp.where(
            same, exact_dot(pick, table), 0.0
        ).astype(jnp.bfloat16)
        return carry

    lax.fori_loop(0, distinct * TILE // height, fill, 0)

    def pieces_wait(sem, count=workers - 1):
        ref = recv.at[0, pl.ds(0, count)]
        pltpu.make_async_copy(ref, ref, sem).wait()

    def home(chunk, owner):
        block = chunk * workers + owner
        row = pl.multiple_of(lax.div(block, columns) * TILE, TILE)
        first = pl.multiple_of(lax.rem(block, columns) * width, 128)
        return pl.ds(row, TILE), pl.ds(first, width)

    mine = lax.rem(me, half)
    def forward_all(chunk):
        pieces_wait(far_recv_sem.at[chunk], half - 1)

        def forward(step, carry):
            owner = ranked(step)

            @pl.when(owner != mirror(me))
            def _():
                pltpu.make_async_remote_copy(
                    src_ref=out_ref.at[home(chunk, owner)],
                    dst_ref=spare.at[chunk, mine],
                    send_sem=sent_sem.at[0],
                    recv_sem=forward_recv_sem.at[chunk],
                    device_id=mirror(owner),
                    device_id_type=LOGICAL,
                ).start()

            return carry

        lax.fori_loop(0, half, forward, 0)
        spare[chunk, mine] = jnp.zeros((TILE, width), jnp.bfloat16)

    for chunk in range(chunks):
        pieces_wait(recv_sem.at[chunk])
        got = recv[chunk].reshape(workers * TILE, width)

        def blend(step, carry):
            result = exact_dot(
                spread[pl.ds(pl.multiple_of(step * height, height), height), :], got
            )
            mixed[chunk, pl.ds(step * (height // TILE), height // TILE)] = result.astype(
                jnp.bfloat16
            ).reshape(height // TILE, TILE, width)
            return carry

        lax.fori_loop(0, distinct * TILE // height, blend, 0)
        out_ref[home(chunk, me)] = mixed[chunk, mine]

        def back(step, absent, sem):
            device = ranked(step)

            @pl.when(device != absent)
            def _():
                pltpu.make_async_remote_copy(
                    src_ref=mixed.at[chunk, lax.rem(device, half)],
                    dst_ref=out_ref.at[home(chunk, me)],
                    send_sem=sent_sem.at[0],
                    recv_sem=sem.at[chunk],
                    device_id=device,
                    device_id_type=LOGICAL,
                ).start()

        def back_far(step, carry):
            last = chunk == chunks - 1
            back(step, me if last else mirror(me), back_recv_sem if last else far_recv_sem)
            return carry

        def back_near(step, carry):
            back(step, me, back_recv_sem)
            return carry

        if chunk == chunks - 1:
            lax.fori_loop(0, half // 2, back_far, 0)
            lax.fori_loop(half, workers, back_near, 0)
            for earlier in range(chunks - 1):
                forward_all(earlier)
            lax.fori_loop(half // 2, half, back_far, 0)
        else:
            lax.fori_loop(half, workers, back_near, 0)
            lax.fori_loop(0, half, back_far, 0)

    for chunk in range(chunks - 1):
        pieces_wait(forward_recv_sem.at[chunk], half - 1)
        total = jnp.zeros((TILE, width), jnp.float32)
        for k in range(half):
            piece = spare[chunk, k].astype(jnp.float32)
            total = total - piece if k % 2 else total + piece
        total = jnp.where(lax.rem(me, 2) == 1, total, -total)
        out_ref[home(chunk, mirror(me))] = total.astype(jnp.bfloat16)

    for chunk in range(chunks):
        last = chunk == chunks - 1
        for count in (workers - 1, workers - 1 if last else workers - 2):
            pieces_wait(sent_sem.at[0], count)
        if not last:
            pieces_wait(sent_sem.at[0], half - 1)
        pieces_wait(back_recv_sem.at[chunk], workers - 1 if last else half - 1)


def store(mixed_ref, moment_ref, mixed_hbm, moment_hbm, sem):
    copies = [
        pltpu.make_async_copy(mixed_ref, mixed_hbm, sem.at[0]),
        pltpu.make_async_copy(moment_ref, moment_hbm, sem.at[1]),
    ]
    for copy in copies:
        copy.start()
    for copy in copies:
        copy.wait()


def shards(sizes, hidden_acts, output_grad, weights, momentum, worker_of_slot, round_shift):
    hidden = hidden_acts.reshape(hidden_acts.shape[-2:])
    grad_out = output_grad.reshape(output_grad.shape[-2:]).T
    weight = weights.reshape(weights.shape[-2:])
    moment = momentum.reshape(momentum.shape[-2:])
    workers = sizes[0] * sizes[1] * sizes[2]
    tokens, features = hidden.shape
    rows = weight.shape[0]
    parts = rows // TILE
    width = max(128, features // workers)
    columns = features // width
    chunks = parts * columns // workers
    distinct = workers // 2
    groups = columns // GROUP
    anywhere = pl.BlockSpec(memory_space=pl.ANY)
    vmem = pl.BlockSpec(memory_space=pltpu.VMEM)
    half = jnp.bfloat16
    mixed, new_moment = pl.pallas_call(
        functools.partial(kernel, sizes),
        out_shape=[pltpu.VMEM((rows, features), half)] * 2,
        in_specs=[anywhere] * 6,
        out_specs=[vmem, vmem],
        scratch_shapes=[
            pltpu.VMEM((groups, tokens, GROUP * width), half),
            pltpu.VMEM((rows, tokens), half),
            pltpu.VMEM((groups, rows, GROUP * width), half),
            pltpu.VMEM((groups, rows, GROUP * width), half),
            pltpu.VMEM((1, workers), jnp.int32),
            pltpu.SMEM(round_shift.shape, jnp.int32),
            pltpu.VMEM((parts, columns, TILE, width), half),
            pltpu.VMEM((chunks, workers, TILE, width), half),
            pltpu.VMEM((chunks, distinct, TILE, width), half),
            pltpu.VMEM((distinct * TILE, workers * TILE), half),
            pltpu.SemaphoreType.DMA((GROUP + 1 + pl.cdiv(groups - 2, BANK),)),
            pltpu.SemaphoreType.DMA((1,)),
            pltpu.SemaphoreType.REGULAR,
            pltpu.SemaphoreType.REGULAR,
            pltpu.SemaphoreType.REGULAR,
            pltpu.SemaphoreType.DMA((1,)),
            pltpu.SemaphoreType.DMA((chunks,)),
            pltpu.SemaphoreType.DMA((chunks,)),
            pltpu.SemaphoreType.DMA((max(1, chunks - 1),)),
            pltpu.SemaphoreType.DMA((max(1, chunks - 1),)),
            pltpu.VMEM((max(1, chunks - 1), distinct, TILE, width), half),
        ],
        compiler_params=pltpu.CompilerParams(
            collective_id=0, has_side_effects=True, vmem_limit_bytes=60 * 1024 * 1024
        ),
        name="step_and_gossip",
    )(hidden, grad_out, weight, moment, worker_of_slot.reshape(1, workers), round_shift)
    mixed, new_moment = pl.pallas_call(
        store,
        out_shape=[jax.ShapeDtypeStruct((rows, features), half)] * 2,
        in_specs=[anywhere, anywhere],
        out_specs=[anywhere, anywhere],
        scratch_shapes=[pltpu.SemaphoreType.DMA((2,))],
        name="store",
    )(
        pltpu.with_memory_space_constraint(mixed, pltpu.VMEM),
        pltpu.with_memory_space_constraint(new_moment, pltpu.VMEM),
    )
    return (mixed.reshape(weights.shape), new_moment.reshape(momentum.shape))


def solution(mesh):
    sizes = (mesh.shape["gx"], mesh.shape["gy"], mesh.shape["gz"])
    placed = (
        P("gz", "gy", "gx", None, None),
        P("gz", "gy", "gx", None, None),
        P("gz", "gy", "gx", None, None),
        P("gz", "gy", "gx", None, None),
        P(),
        P(),
    )
    return jax.shard_map(
        functools.partial(shards, sizes),
        mesh=mesh,
        in_specs=placed,
        out_specs=(P("gx", "gy", "gz", None, None), P("gz", "gy", "gx", None, None)),
        check_vma=False,
    )
```

```python
import functools

import jax
import jax.numpy as jnp
from jax import lax
from jax.experimental import pallas as pl
from jax.experimental.pallas import tpu as pltpu
from jax.sharding import PartitionSpec as P

learn_rate = 0.01
beta_keep = 0.9
TILE = 16
GROUP = 2
BANK = 4
LOGICAL = pl.DeviceIdType.LOGICAL


def iota(shape, axis):
    return lax.broadcasted_iota(jnp.int32, shape, axis)


def ones_where(mask):
    return jnp.where(mask, 1.0, 0.0).astype(jnp.bfloat16)


def exact_dot(a, b):
    return jnp.dot(a, b, preferred_element_type=jnp.float32)


def kernel(
    sizes,
    hidden_hbm,
    grad_hbm,
    weight_hbm,
    moment_hbm,
    held_hbm,
    shift_hbm,
    out_ref,
    new_moment_ref,
    hidden,
    grad_ref,
    weight,
    moment,
    held_ref,
    shift_ref,
    stage,
    recv,
    mixed,
    spread,
    load_sem,
    table_sem,
    line_sem,
    hub_sem,
    all_sem,
    sent_sem,
    recv_sem,
    back_recv_sem,
    far_recv_sem,
    forward_recv_sem,
    spare,
):
    size_x, size_y, size_z = sizes
    workers = size_x * size_y * size_z
    width = stage.shape[-1]
    groups, _, span = hidden.shape
    columns = stage.shape[1]
    parts = out_ref.shape[0] // TILE
    chunks = recv.shape[0]
    rounds = shift_ref.shape[0]
    my_x, my_y, my_z = lax.axis_index("gx"), lax.axis_index("gy"), lax.axis_index("gz")
    me = (my_x * size_y + my_y) * size_z + my_z
    slot = my_x + size_x * (my_y + size_y * my_z)

    plane = size_y * size_z
    half = workers // 2
    side = lax.div(me, half)
    lines = plane // GROUP
    layers = (half if columns == workers else columns) // plane
    my_line = lax.div(lax.rem(me, plane), GROUP)

    def ranked(step):
        far = 1 - lax.div(step, half)
        turn = (side ^ far) * (size_x - 1)
        layer = lax.div(lax.rem(step, half), plane) ^ turn
        turn_step = lax.rem(step, plane)
        low = ((me & (plane - 1)) ^ (plane - 1 - turn_step)) & (plane - 2)
        return layer * plane + low + (turn_step & 1)

    def pair(group):
        side_groups = layers * lines
        order = lax.rem(group, side_groups)
        turn = my_line ^ ((lines - lax.div(order, layers)) & (lines - 1))
        layer = lax.rem(order, layers)
        if columns == workers:
            far = 1 - lax.div(group, side_groups)
            layer = layer ^ my_x ^ (far * (size_x - 1))
        return layer * lines + turn

    def bank(group):
        return GROUP + lax.div(group + BANK - 2, BANK)

    def loads(group, first=0, count=GROUP, sem=None):
        place = pair(group)
        take = count * width
        cut = pl.ds(pl.multiple_of(place * span + first * width, 128), take)
        return [
            pltpu.make_async_copy(
                source.at[:, cut],
                kept.at[place, :, pl.ds(first * width, take)],
                load_sem.at[bank(group) if sem is None else sem],
            )
            for source, kept in (
                (hidden_hbm, hidden),
                (moment_hbm, moment),
                (weight_hbm, weight),
            )
        ]

    def load(group, carry):
        for copy in loads(group):
            copy.start()
        return carry

    def single(k):
        return loads(0, k, 1, k)

    barrier = pltpu.get_barrier_semaphore()
    hub = my_x == 0

    def signal(sem, device):
        pl.semaphore_signal(sem, inc=1, device_id=device, device_id_type=LOGICAL)

    def mirror(device):
        return device ^ ((size_x - 1) * plane)

    half_x = size_x // 2
    lead_x = side * (size_x - 1)
    right_lead = my_x == size_x - 1
    leader = jnp.logical_or(hub, right_lead)
    left_inner = jnp.logical_and(my_x > 0, my_x < half_x)
    right_inner = jnp.logical_and(my_x >= half_x, my_x < size_x - 1)
    lead = me ^ ((my_x ^ lead_x) * plane)

    def greet_side(step, carry):
        signal(barrier, me ^ ((step + 1) * plane))
        signal(barrier, me ^ ((step + 1) * plane) ^ 1)
        return carry

    def tell_side(step, carry):
        signal(line_sem, me ^ ((step + 1) * plane))
        return carry

    def greet():
        signal(barrier, mirror(me))
        signal(barrier, mirror(me) ^ 1)
        signal(barrier, me ^ 1)

        @pl.when(jnp.logical_not(leader))
        def _():
            signal(barrier, lead)
            signal(barrier, lead ^ 1)

        @pl.when(hub)
        def _():
            lax.fori_loop(0, half_x - 1, greet_side, 0)
            lax.fori_loop(0, lines - 1, greet_hub, 0)

    others = 2 * (half_x - 1)
    expected = 3 + jnp.where(leader, others, 0) + jnp.where(left_inner, 2, 0)
    expected = expected + jnp.where(hub, lines - 1, 0)

    def greet_hub(step, carry):
        signal(barrier, me ^ ((step + 1) * GROUP))
        return carry

    def tell_hub(step, carry):
        signal(hub_sem, me ^ ((step + 1) * GROUP))
        return carry

    def tell_line(step, carry):
        signal(all_sem, me ^ ((step + 1) * plane))
        return carry

    grad_copy = pltpu.make_async_copy(grad_hbm, grad_ref, load_sem.at[0])
    table_copies = [
        pltpu.make_async_copy(held_hbm, held_ref, table_sem.at[0]),
        pltpu.make_async_copy(shift_hbm, shift_ref, table_sem.at[0]),
    ]
    grad_copy.start()
    for copy in single(0):
        copy.start()
    greet()
    for k in range(1, GROUP):
        for copy in single(k):
            copy.start()
    lax.fori_loop(1, groups, load, 0)
    for copy in table_copies:
        copy.start()

    def place_of(part, where):
        block = part * columns
        return block // workers, block % workers + where

    def send(part, where):
        chunk, device = place_of(part, where)

        @pl.when(device != me)
        def _():
            pltpu.make_async_remote_copy(
                src_ref=stage.at[part, where],
                dst_ref=recv.at[chunk, slot],
                send_sem=sent_sem.at[0],
                recv_sem=recv_sem.at[chunk],
                device_id=device,
                device_id_type=LOGICAL,
            ).start()

    early = [part for part in range(parts) if place_of(part, 0)[0] == 0]
    late = [part for part in range(parts) if place_of(part, 0)[0] > 0]

    def advance(place, first, count):
        low, take = first * width, count * width
        kept = (place, slice(None), slice(low, low + take))
        velocity = beta_keep * moment[kept].astype(jnp.float32) + exact_dot(
            grad_ref[...], hidden[kept]
        )
        cut = pl.ds(pl.multiple_of(place * span + low, 128), take)
        new_moment_ref[:, cut] = velocity.astype(jnp.bfloat16)
        stepped = (weight[kept].astype(jnp.float32) - learn_rate * velocity).astype(
            jnp.bfloat16
        )
        for k in range(count):
            for part in range(parts):
                stage[part, place * GROUP + first + k] = stepped[
                    part * TILE : (part + 1) * TILE, k * width : (k + 1) * width
                ]

    def compute(group):
        @pl.when((group < 2) | (lax.rem(group + BANK - 2, BANK) == 0))
        def _():
            for step in range(BANK):

                @pl.when((bank(group + step) == bank(group)) & (group + step < groups))
                def _():
                    for copy in loads(group + step):
                        copy.wait()

        advance(pair(group), 0, GROUP)

    def compute_single(k):
        for copy in single(k):
            copy.wait()
        advance(pair(0), k, 1)

    def send_parts(which, group):
        for k in range(GROUP):
            for part in which:
                send(part, pair(group) * GROUP + k)

    def compute_ahead(group, carry):
        compute(group)
        return carry

    def send_ahead(group, carry):
        send_parts(early, group)
        return carry

    def compute_and_send(group, carry):
        compute(group)
        send_parts(early, group - 1)
        return carry

    def send_late(group, carry):
        send_parts(late, group)
        return carry

    grad_copy.wait()
    compute_single(0)
    pl.semaphore_wait(barrier, expected)

    @pl.when(left_inner)
    def _():
        signal(line_sem, lead)

    @pl.when(hub)
    def _():
        pl.semaphore_wait(line_sem, half_x - 1)

    @pl.when(leader)
    def _():
        lax.fori_loop(0, half_x - 1, tell_side, 0)

    @pl.when(hub)
    def _():
        lax.fori_loop(0, lines - 1, tell_hub, 0)

    def send_all(group):
        send_parts(early, jnp.int32(group))
        send_parts(late, jnp.int32(group))

    for k in range(GROUP):
        if k:
            compute_single(k)
        if columns == workers:
            for part in range(parts):
                send(part, pair(0) * GROUP + k)
    compute(jnp.int32(1))

    @pl.when(jnp.logical_not(leader))
    def _():
        pl.semaphore_wait(line_sem, 1)

    @pl.when(right_inner)
    def _():
        signal(line_sem, lead)

    @pl.when(right_lead)
    def _():
        pl.semaphore_wait(line_sem, half_x - 1)

    if half_x > 2:

        @pl.when(right_lead)
        def _():
            lax.fori_loop(0, half_x - 1, tell_side, 0)

        @pl.when(right_inner)
        def _():
            pl.semaphore_wait(line_sem, 1)

    if columns != workers:
        send_all(0)
    send_all(1)
    for group in range(2, layers):
        compute(jnp.int32(group))
        send_all(group)
    ahead = min(layers + 4, groups - 1)
    lax.fori_loop(layers, ahead, compute_ahead, 0)

    @pl.when(hub)
    def _():
        pl.semaphore_wait(hub_sem, lines - 1)
        lax.fori_loop(0, size_x - 1, tell_line, 0)

    @pl.when(jnp.logical_not(hub))
    def _():
        pl.semaphore_wait(all_sem, 1)

    lax.fori_loop(layers, ahead - 1, send_ahead, 0)
    lax.fori_loop(ahead, groups, compute_and_send, 0)
    send_parts(early, jnp.int32(groups - 1))
    if late:
        lax.fori_loop(layers, groups, send_late, 0)
    for chunk in range(chunks):
        block = chunk * workers + me
        recv[chunk, slot] = stage[lax.div(block, columns), lax.rem(block, columns)]
    for copy in table_copies:
        copy.wait()

    square = (workers, workers)
    gap = lax.rem(iota(square, 0) - iota(square, 1) + workers, workers)
    level = jnp.full(square, -1, jnp.int32)
    for power in range(workers.bit_length() - 1):
        level = jnp.where(gap == 1 << power, power, level)
    table = ones_where(held_ref[...] == iota(square, 0))
    for step in range(rounds):
        turn = ones_where((gap == 0) | (level == shift_ref[step]))
        table = exact_dot(turn, table).astype(jnp.bfloat16)
    distinct = workers // 2
    table = (table[:distinct].astype(jnp.float32) * 0.5**rounds).astype(jnp.bfloat16)
    wide = (workers, workers * TILE)
    table = exact_dot(table, ones_where(iota(wide, 1) // TILE == iota(wide, 0))).astype(
        jnp.bfloat16
    )
    height = min(256, distinct * TILE)

    def fill(step, carry):
        tall = (height, distinct)
        pick = ones_where((iota(tall, 0) + step * height) // TILE == iota(tall, 1))
        full = (height, workers * TILE)
        same = iota(full, 0) % TILE == iota(full, 1) % TILE
        spread[pl.ds(pl.multiple_of(step * height, height), height), :] = jnp.where(
            same, exact_dot(pick, table), 0.0
        ).astype(jnp.bfloat16)
        return carry

    lax.fori_loop(0, distinct * TILE // height, fill, 0)

    def pieces_wait(sem, count=workers - 1):
        ref = recv.at[0, pl.ds(0, count)]
        pltpu.make_async_copy(ref, ref, sem).wait()

    def home(chunk, owner):
        block = chunk * workers + owner
        row = pl.multiple_of(lax.div(block, columns) * TILE, TILE)
        first = pl.multiple_of(lax.rem(block, columns) * width, 128)
        return pl.ds(row, TILE), pl.ds(first, width)

    mine = lax.rem(me, half)
    def forward_all(chunk):
        pieces_wait(far_recv_sem.at[chunk], half - 1)

        def forward(step, carry):
            owner = ranked(step)

            @pl.when(owner != mirror(me))
            def _():
                pltpu.make_async_remote_copy(
                    src_ref=out_ref.at[home(chunk, owner)],
                    dst_ref=spare.at[chunk, mine],
                    send_sem=sent_sem.at[0],
                    recv_sem=forward_recv_sem.at[chunk],
                    device_id=mirror(owner),
                    device_id_type=LOGICAL,
                ).start()

            return carry

        lax.fori_loop(0, half, forward, 0)
        spare[chunk, mine] = jnp.zeros((TILE, width), jnp.bfloat16)

    for chunk in range(chunks):
        pieces_wait(recv_sem.at[chunk])
        got = recv[chunk].reshape(workers * TILE, width)

        def blend(step, carry):
            result = exact_dot(
                spread[pl.ds(pl.multiple_of(step * height, height), height), :], got
            )
            mixed[chunk, pl.ds(step * (height // TILE), height // TILE)] = result.astype(
                jnp.bfloat16
            ).reshape(height // TILE, TILE, width)
            return carry

        lax.fori_loop(0, distinct * TILE // height, blend, 0)
        out_ref[home(chunk, me)] = mixed[chunk, mine]

        def back(step, absent, sem):
            device = ranked(step)

            @pl.when(device != absent)
            def _():
                pltpu.make_async_remote_copy(
                    src_ref=mixed.at[chunk, lax.rem(device, half)],
                    dst_ref=out_ref.at[home(chunk, me)],
                    send_sem=sent_sem.at[0],
                    recv_sem=sem.at[chunk],
                    device_id=device,
                    device_id_type=LOGICAL,
                ).start()

        def back_far(step, carry):
            last = chunk == chunks - 1
            back(step, me if last else mirror(me), back_recv_sem if last else far_recv_sem)
            return carry

        def back_near(step, carry):
            back(step, me, back_recv_sem)
            return carry

        if chunk == chunks - 1:
            lax.fori_loop(0, half // 2, back_far, 0)
            lax.fori_loop(half, workers, back_near, 0)
            for earlier in range(chunks - 1):
                forward_all(earlier)
            lax.fori_loop(half // 2, half, back_far, 0)
        else:
            lax.fori_loop(half, workers, back_near, 0)
            lax.fori_loop(0, half, back_far, 0)

    for chunk in range(chunks - 1):
        pieces_wait(forward_recv_sem.at[chunk], half - 1)
        total = jnp.zeros((TILE, width), jnp.float32)
        for k in range(half):
            piece = spare[chunk, k].astype(jnp.float32)
            total = total - piece if k % 2 else total + piece
        total = jnp.where(lax.rem(me, 2) == 1, total, -total)
        out_ref[home(chunk, mirror(me))] = total.astype(jnp.bfloat16)

    for chunk in range(chunks):
        last = chunk == chunks - 1
        for count in (workers - 1, workers - 1 if last else workers - 2):
            pieces_wait(sent_sem.at[0], count)
        if not last:
            pieces_wait(sent_sem.at[0], half - 1)
        pieces_wait(back_recv_sem.at[chunk], workers - 1 if last else half - 1)


def store(mixed_ref, moment_ref, mixed_hbm, moment_hbm, sem):
    copies = [
        pltpu.make_async_copy(mixed_ref, mixed_hbm, sem.at[0]),
        pltpu.make_async_copy(moment_ref, moment_hbm, sem.at[1]),
    ]
    for copy in copies:
        copy.start()
    for copy in copies:
        copy.wait()


def shards(sizes, hidden_acts, output_grad, weights, momentum, worker_of_slot, round_shift):
    hidden = hidden_acts.reshape(hidden_acts.shape[-2:])
    grad_out = output_grad.reshape(output_grad.shape[-2:]).T
    weight = weights.reshape(weights.shape[-2:])
    moment = momentum.reshape(momentum.shape[-2:])
    workers = sizes[0] * sizes[1] * sizes[2]
    tokens, features = hidden.shape
    rows = weight.shape[0]
    parts = rows // TILE
    width = max(128, features // workers)
    columns = features // width
    chunks = parts * columns // workers
    distinct = workers // 2
    groups = columns // GROUP
    anywhere = pl.BlockSpec(memory_space=pl.ANY)
    vmem = pl.BlockSpec(memory_space=pltpu.VMEM)
    half = jnp.bfloat16
    mixed, new_moment = pl.pallas_call(
        functools.partial(kernel, sizes),
        out_shape=[pltpu.VMEM((rows, features), half)] * 2,
        in_specs=[anywhere] * 6,
        out_specs=[vmem, vmem],
        scratch_shapes=[
            pltpu.VMEM((groups, tokens, GROUP * width), half),
            pltpu.VMEM((rows, tokens), half),
            pltpu.VMEM((groups, rows, GROUP * width), half),
            pltpu.VMEM((groups, rows, GROUP * width), half),
            pltpu.VMEM((1, workers), jnp.int32),
            pltpu.SMEM(round_shift.shape, jnp.int32),
            pltpu.VMEM((parts, columns, TILE, width), half),
            pltpu.VMEM((chunks, workers, TILE, width), half),
            pltpu.VMEM((chunks, distinct, TILE, width), half),
            pltpu.VMEM((distinct * TILE, workers * TILE), half),
            pltpu.SemaphoreType.DMA((GROUP + 1 + pl.cdiv(groups - 2, BANK),)),
            pltpu.SemaphoreType.DMA((1,)),
            pltpu.SemaphoreType.REGULAR,
            pltpu.SemaphoreType.REGULAR,
            pltpu.SemaphoreType.REGULAR,
            pltpu.SemaphoreType.DMA((1,)),
            pltpu.SemaphoreType.DMA((chunks,)),
            pltpu.SemaphoreType.DMA((chunks,)),
            pltpu.SemaphoreType.DMA((max(1, chunks - 1),)),
            pltpu.SemaphoreType.DMA((max(1, chunks - 1),)),
            pltpu.VMEM((max(1, chunks - 1), distinct, TILE, width), half),
        ],
        compiler_params=pltpu.CompilerParams(
            collective_id=0, has_side_effects=True, vmem_limit_bytes=60 * 1024 * 1024
        ),
        name="step_and_gossip",
    )(hidden, grad_out, weight, moment, worker_of_slot.reshape(1, workers), round_shift)
    mixed, new_moment = pl.pallas_call(
        store,
        out_shape=[jax.ShapeDtypeStruct((rows, features), half)] * 2,
        in_specs=[anywhere, anywhere],
        out_specs=[anywhere, anywhere],
        scratch_shapes=[pltpu.SemaphoreType.DMA((2,))],
        name="store",
    )(
        pltpu.with_memory_space_constraint(mixed, pltpu.VMEM),
        pltpu.with_memory_space_constraint(new_moment, pltpu.VMEM),
    )
    return (mixed.reshape(weights.shape), new_moment.reshape(momentum.shape))


def solution(mesh):
    sizes = (mesh.shape["gx"], mesh.shape["gy"], mesh.shape["gz"])
    placed = (
        P("gz", "gy", "gx", None, None),
        P("gz", "gy", "gx", None, None),
        P("gz", "gy", "gx", None, None),
        P("gz", "gy", "gx", None, None),
        P(),
        P(),
    )
    return jax.shard_map(
        functools.partial(shards, sizes),
        mesh=mesh,
        in_specs=placed,
        out_specs=(P("gx", "gy", "gz", None, None), P("gz", "gy", "gx", None, None)),
        check_vma=False,
    )
```

```python
import functools

import jax
import jax.numpy as jnp
from jax import lax
from jax.experimental import pallas as pl
from jax.experimental.pallas import tpu as pltpu
from jax.sharding import PartitionSpec as P

learn_rate = 0.01
beta_keep = 0.9
TILE = 16
GROUP = 2
BANK = 4
SLICES = 4
LOGICAL = pl.DeviceIdType.LOGICAL


def iota(shape, axis):
    return lax.broadcasted_iota(jnp.int32, shape, axis)


def ones_where(mask):
    return jnp.where(mask, 1.0, 0.0).astype(jnp.bfloat16)


def exact_dot(a, b):
    return jnp.dot(a, b, preferred_element_type=jnp.float32)


def kernel(
    sizes,
    hidden_hbm,
    grad_hbm,
    weight_hbm,
    moment_hbm,
    held_hbm,
    shift_hbm,
    out_ref,
    new_moment_ref,
    hidden,
    grad_ref,
    weight,
    moment,
    held_ref,
    shift_ref,
    stage,
    recv,
    mixed,
    spread,
    load_sem,
    table_sem,
    line_sem,
    hub_sem,
    all_sem,
    sent_sem,
    recv_sem,
    back_recv_sem,
    far_recv_sem,
    forward_recv_sem,
    spare,
):
    size_x, size_y, size_z = sizes
    workers = size_x * size_y * size_z
    width = stage.shape[-1]
    groups, _, span = hidden.shape
    columns = stage.shape[1]
    parts = out_ref.shape[0] // TILE
    chunks = recv.shape[0]
    rounds = shift_ref.shape[0]
    my_x, my_y, my_z = lax.axis_index("gx"), lax.axis_index("gy"), lax.axis_index("gz")
    me = (my_x * size_y + my_y) * size_z + my_z
    slot = my_x + size_x * (my_y + size_y * my_z)

    plane = size_y * size_z
    half = workers // 2
    side = lax.div(me, half)
    lines = plane // GROUP
    layers = (half if columns == workers else columns) // plane
    my_line = lax.div(lax.rem(me, plane), GROUP)

    def ranked(step):
        far = 1 - lax.div(step, half)
        turn = (side ^ far) * (size_x - 1)
        layer = lax.div(lax.rem(step, half), plane) ^ turn
        turn_step = lax.rem(step, plane)
        low = ((me & (plane - 1)) ^ (plane - 1 - turn_step)) & (plane - 2)
        return layer * plane + low + (turn_step & 1)

    def pair(group):
        side_groups = layers * lines
        order = lax.rem(group, side_groups)
        turn = my_line ^ ((lines - lax.div(order, layers)) & (lines - 1))
        layer = lax.rem(order, layers)
        if columns == workers:
            far = 1 - lax.div(group, side_groups)
            layer = layer ^ my_x ^ (far * (size_x - 1))
        return layer * lines + turn

    def bank(group):
        return GROUP + lax.div(group + BANK - 2, BANK)

    def loads(group):
        place = pair(group)
        cut = pl.ds(pl.multiple_of(place * span, 128), span)
        return [
            pltpu.make_async_copy(
                source.at[:, cut], kept.at[place], load_sem.at[bank(group)]
            )
            for source, kept in (
                (hidden_hbm, hidden),
                (moment_hbm, moment),
                (weight_hbm, weight),
            )
        ]

    def load(group, carry):
        for copy in loads(group):
            copy.start()
        return carry

    def single(k):
        place = pair(0)
        cut = pl.ds(pl.multiple_of(place * span + k * width, 128), width)
        lanes = pl.ds(k * width, width)
        tokens = hidden.shape[1] // SLICES
        copies = []
        for step in range(SLICES):
            some = pl.ds(step * tokens, tokens)
            source, kept = hidden_hbm.at[some, cut], hidden.at[place, some, lanes]
            copies.append(pltpu.make_async_copy(source, kept, load_sem.at[k]))
        for source, kept in ((moment_hbm, moment), (weight_hbm, weight)):
            copies.append(
                pltpu.make_async_copy(
                    source.at[:, cut], kept.at[place, :, lanes], load_sem.at[k]
                )
            )
        return copies

    barrier = pltpu.get_barrier_semaphore()
    hub = my_x == 0

    def signal(sem, device):
        pl.semaphore_signal(sem, inc=1, device_id=device, device_id_type=LOGICAL)

    def mirror(device):
        return device ^ ((size_x - 1) * plane)

    half_x = size_x // 2
    lead_x = side * (size_x - 1)
    right_lead = my_x == size_x - 1
    leader = jnp.logical_or(hub, right_lead)
    left_inner = jnp.logical_and(my_x > 0, my_x < half_x)
    right_inner = jnp.logical_and(my_x >= half_x, my_x < size_x - 1)
    lead = me ^ ((my_x ^ lead_x) * plane)

    def greet_side(step, carry):
        signal(barrier, me ^ ((step + 1) * plane))
        signal(barrier, me ^ ((step + 1) * plane) ^ 1)
        return carry

    def tell_side(step, carry):
        signal(line_sem, me ^ ((step + 1) * plane))
        return carry

    def greet():
        signal(barrier, mirror(me))
        signal(barrier, mirror(me) ^ 1)
        signal(barrier, me ^ 1)

        @pl.when(jnp.logical_not(leader))
        def _():
            signal(barrier, lead)
            signal(barrier, lead ^ 1)

        @pl.when(hub)
        def _():
            lax.fori_loop(0, half_x - 1, greet_side, 0)
            lax.fori_loop(0, lines - 1, greet_hub, 0)

    others = 2 * (half_x - 1)
    expected = 3 + jnp.where(leader, others, 0) + jnp.where(left_inner, 2, 0)
    expected = expected + jnp.where(hub, lines - 1, 0)

    def greet_hub(step, carry):
        signal(barrier, me ^ ((step + 1) * GROUP))
        return carry

    def tell_hub(step, carry):
        signal(hub_sem, me ^ ((step + 1) * GROUP))
        return carry

    def tell_line(step, carry):
        signal(all_sem, me ^ ((step + 1) * plane))
        return carry

    grad_copy = pltpu.make_async_copy(grad_hbm, grad_ref, load_sem.at[0])
    table_copies = [
        pltpu.make_async_copy(held_hbm, held_ref, table_sem.at[0]),
        pltpu.make_async_copy(shift_hbm, shift_ref, table_sem.at[0]),
    ]
    grad_copy.start()
    for copy in single(0):
        copy.start()
    greet()
    for k in range(1, GROUP):
        for copy in single(k):
            copy.start()
    lax.fori_loop(1, groups, load, 0)
    for copy in table_copies:
        copy.start()

    def place_of(part, where):
        block = part * columns
        return block // workers, block % workers + where

    def send(part, where):
        chunk, device = place_of(part, where)

        @pl.when(device != me)
        def _():
            pltpu.make_async_remote_copy(
                src_ref=stage.at[part, where],
                dst_ref=recv.at[chunk, slot],
                send_sem=sent_sem.at[0],
                recv_sem=recv_sem.at[chunk],
                device_id=device,
                device_id_type=LOGICAL,
            ).start()

    early = [part for part in range(parts) if place_of(part, 0)[0] == 0]
    late = [part for part in range(parts) if place_of(part, 0)[0] > 0]

    def advance(place, first, count):
        low, take = first * width, count * width
        kept = (place, slice(None), slice(low, low + take))
        velocity = beta_keep * moment[kept].astype(jnp.float32) + exact_dot(
            grad_ref[...], hidden[kept]
        )
        cut = pl.ds(pl.multiple_of(place * span + low, 128), take)
        new_moment_ref[:, cut] = velocity.astype(jnp.bfloat16)
        stepped = (weight[kept].astype(jnp.float32) - learn_rate * velocity).astype(
            jnp.bfloat16
        )
        for k in range(count):
            for part in range(parts):
                stage[part, place * GROUP + first + k] = stepped[
                    part * TILE : (part + 1) * TILE, k * width : (k + 1) * width
                ]

    def compute(group):
        @pl.when((group < 2) | (lax.rem(group + BANK - 2, BANK) == 0))
        def _():
            for step in range(BANK):

                @pl.when((bank(group + step) == bank(group)) & (group + step < groups))
                def _():
                    for copy in loads(group + step):
                        copy.wait()

        advance(pair(group), 0, GROUP)

    def compute_single(k):
        for copy in single(k):
            copy.wait()
        advance(pair(0), k, 1)

    def send_parts(which, group):
        for k in range(GROUP):
            for part in which:
                send(part, pair(group) * GROUP + k)

    def compute_ahead(group, carry):
        compute(group)
        return carry

    def send_ahead(group, carry):
        send_parts(early, group)
        return carry

    def compute_and_send(group, carry):
        compute(group)
        send_parts(early, group - 1)
        return carry

    def send_late(group, carry):
        send_parts(late, group)
        return carry

    grad_copy.wait()
    compute_single(0)
    pl.semaphore_wait(barrier, expected)

    @pl.when(left_inner)
    def _():
        signal(line_sem, lead)

    @pl.when(hub)
    def _():
        pl.semaphore_wait(line_sem, half_x - 1)

    @pl.when(leader)
    def _():
        lax.fori_loop(0, half_x - 1, tell_side, 0)

    @pl.when(hub)
    def _():
        lax.fori_loop(0, lines - 1, tell_hub, 0)

    def send_all(group):
        send_parts(early, jnp.int32(group))
        send_parts(late, jnp.int32(group))

    for k in range(GROUP):
        if k:
            compute_single(k)
        if columns == workers:
            for part in range(parts):
                send(part, pair(0) * GROUP + k)
    compute(jnp.int32(1))

    @pl.when(jnp.logical_not(leader))
    def _():
        pl.semaphore_wait(line_sem, 1)

    @pl.when(right_inner)
    def _():
        signal(line_sem, lead)

    @pl.when(right_lead)
    def _():
        pl.semaphore_wait(line_sem, half_x - 1)

    if half_x > 2:

        @pl.when(right_lead)
        def _():
            lax.fori_loop(0, half_x - 1, tell_side, 0)

        @pl.when(right_inner)
        def _():
            pl.semaphore_wait(line_sem, 1)

    if columns != workers:
        send_all(0)
    send_all(1)
    for group in range(2, layers):
        compute(jnp.int32(group))
        send_all(group)
    ahead = min(layers + 4, groups - 1)
    lax.fori_loop(layers, ahead, compute_ahead, 0)

    @pl.when(hub)
    def _():
        pl.semaphore_wait(hub_sem, lines - 1)
        lax.fori_loop(0, size_x - 1, tell_line, 0)

    @pl.when(jnp.logical_not(hub))
    def _():
        pl.semaphore_wait(all_sem, 1)

    lax.fori_loop(layers, ahead - 1, send_ahead, 0)
    lax.fori_loop(ahead, groups, compute_and_send, 0)
    send_parts(early, jnp.int32(groups - 1))
    if late:
        lax.fori_loop(layers, groups, send_late, 0)
    for chunk in range(chunks):
        block = chunk * workers + me
        recv[chunk, slot] = stage[lax.div(block, columns), lax.rem(block, columns)]
    for copy in table_copies:
        copy.wait()

    square = (workers, workers)
    gap = lax.rem(iota(square, 0) - iota(square, 1) + workers, workers)
    level = jnp.full(square, -1, jnp.int32)
    for power in range(workers.bit_length() - 1):
        level = jnp.where(gap == 1 << power, power, level)
    table = ones_where(held_ref[...] == iota(square, 0))
    for step in range(rounds):
        turn = ones_where((gap == 0) | (level == shift_ref[step]))
        table = exact_dot(turn, table).astype(jnp.bfloat16)
    distinct = workers // 2
    table = (table[:distinct].astype(jnp.float32) * 0.5**rounds).astype(jnp.bfloat16)
    wide = (workers, workers * TILE)
    table = exact_dot(table, ones_where(iota(wide, 1) // TILE == iota(wide, 0))).astype(
        jnp.bfloat16
    )
    height = min(256, distinct * TILE)

    def fill(step, carry):
        tall = (height, distinct)
        pick = ones_where((iota(tall, 0) + step * height) // TILE == iota(tall, 1))
        full = (height, workers * TILE)
        same = iota(full, 0) % TILE == iota(full, 1) % TILE
        spread[pl.ds(pl.multiple_of(step * height, height), height), :] = jnp.where(
            same, exact_dot(pick, table), 0.0
        ).astype(jnp.bfloat16)
        return carry

    lax.fori_loop(0, distinct * TILE // height, fill, 0)

    def pieces_wait(sem, count=workers - 1):
        ref = recv.at[0, pl.ds(0, count)]
        pltpu.make_async_copy(ref, ref, sem).wait()

    def home(chunk, owner):
        block = chunk * workers + owner
        row = pl.multiple_of(lax.div(block, columns) * TILE, TILE)
        first = pl.multiple_of(lax.rem(block, columns) * width, 128)
        return pl.ds(row, TILE), pl.ds(first, width)

    mine = lax.rem(me, half)
    def forward_all(chunk):
        pieces_wait(far_recv_sem.at[chunk], half - 1)

        def forward(step, carry):
            owner = ranked(step)

            @pl.when(owner != mirror(me))
            def _():
                pltpu.make_async_remote_copy(
                    src_ref=out_ref.at[home(chunk, owner)],
                    dst_ref=spare.at[chunk, mine],
                    send_sem=sent_sem.at[0],
                    recv_sem=forward_recv_sem.at[chunk],
                    device_id=mirror(owner),
                    device_id_type=LOGICAL,
                ).start()

            return carry

        lax.fori_loop(0, half, forward, 0)
        spare[chunk, mine] = jnp.zeros((TILE, width), jnp.bfloat16)

    for chunk in range(chunks):
        pieces_wait(recv_sem.at[chunk])
        got = recv[chunk].reshape(workers * TILE, width)

        def blend(step, carry):
            result = exact_dot(
                spread[pl.ds(pl.multiple_of(step * height, height), height), :], got
            )
            mixed[chunk, pl.ds(step * (height // TILE), height // TILE)] = result.astype(
                jnp.bfloat16
            ).reshape(height // TILE, TILE, width)
            return carry

        lax.fori_loop(0, distinct * TILE // height, blend, 0)
        out_ref[home(chunk, me)] = mixed[chunk, mine]

        def back(step, absent, sem):
            device = ranked(step)

            @pl.when(device != absent)
            def _():
                pltpu.make_async_remote_copy(
                    src_ref=mixed.at[chunk, lax.rem(device, half)],
                    dst_ref=out_ref.at[home(chunk, me)],
                    send_sem=sent_sem.at[0],
                    recv_sem=sem.at[chunk],
                    device_id=device,
                    device_id_type=LOGICAL,
                ).start()

        def back_far(step, carry):
            last = chunk == chunks - 1
            back(step, me if last else mirror(me), back_recv_sem if last else far_recv_sem)
            return carry

        def back_near(step, carry):
            back(step, me, back_recv_sem)
            return carry

        if chunk == chunks - 1:
            lax.fori_loop(0, half // 2, back_far, 0)
            lax.fori_loop(half, workers, back_near, 0)
            for earlier in range(chunks - 1):
                forward_all(earlier)
            lax.fori_loop(half // 2, half, back_far, 0)
        else:
            lax.fori_loop(half, workers, back_near, 0)
            lax.fori_loop(0, half, back_far, 0)

    for chunk in range(chunks - 1):
        pieces_wait(forward_recv_sem.at[chunk], half - 1)
        total = jnp.zeros((TILE, width), jnp.float32)
        for k in range(half):
            piece = spare[chunk, k].astype(jnp.float32)
            total = total - piece if k % 2 else total + piece
        total = jnp.where(lax.rem(me, 2) == 1, total, -total)
        out_ref[home(chunk, mirror(me))] = total.astype(jnp.bfloat16)

    for chunk in range(chunks):
        last = chunk == chunks - 1
        for count in (workers - 1, workers - 1 if last else workers - 2):
            pieces_wait(sent_sem.at[0], count)
        if not last:
            pieces_wait(sent_sem.at[0], half - 1)
        pieces_wait(back_recv_sem.at[chunk], workers - 1 if last else half - 1)


def store(mixed_ref, moment_ref, mixed_hbm, moment_hbm, sem):
    copies = [
        pltpu.make_async_copy(mixed_ref, mixed_hbm, sem.at[0]),
        pltpu.make_async_copy(moment_ref, moment_hbm, sem.at[1]),
    ]
    for copy in copies:
        copy.start()
    for copy in copies:
        copy.wait()


def shards(sizes, hidden_acts, output_grad, weights, momentum, worker_of_slot, round_shift):
    hidden = hidden_acts.reshape(hidden_acts.shape[-2:])
    grad_out = output_grad.reshape(output_grad.shape[-2:]).T
    weight = weights.reshape(weights.shape[-2:])
    moment = momentum.reshape(momentum.shape[-2:])
    workers = sizes[0] * sizes[1] * sizes[2]
    tokens, features = hidden.shape
    rows = weight.shape[0]
    parts = rows // TILE
    width = max(128, features // workers)
    columns = features // width
    chunks = parts * columns // workers
    distinct = workers // 2
    groups = columns // GROUP
    anywhere = pl.BlockSpec(memory_space=pl.ANY)
    vmem = pl.BlockSpec(memory_space=pltpu.VMEM)
    half = jnp.bfloat16
    mixed, new_moment = pl.pallas_call(
        functools.partial(kernel, sizes),
        out_shape=[pltpu.VMEM((rows, features), half)] * 2,
        in_specs=[anywhere] * 6,
        out_specs=[vmem, vmem],
        scratch_shapes=[
            pltpu.VMEM((groups, tokens, GROUP * width), half),
            pltpu.VMEM((rows, tokens), half),
            pltpu.VMEM((groups, rows, GROUP * width), half),
            pltpu.VMEM((groups, rows, GROUP * width), half),
            pltpu.VMEM((1, workers), jnp.int32),
            pltpu.SMEM(round_shift.shape, jnp.int32),
            pltpu.VMEM((parts, columns, TILE, width), half),
            pltpu.VMEM((chunks, workers, TILE, width), half),
            pltpu.VMEM((chunks, distinct, TILE, width), half),
            pltpu.VMEM((distinct * TILE, workers * TILE), half),
            pltpu.SemaphoreType.DMA((GROUP + 1 + pl.cdiv(groups - 2, BANK),)),
            pltpu.SemaphoreType.DMA((1,)),
            pltpu.SemaphoreType.REGULAR,
            pltpu.SemaphoreType.REGULAR,
            pltpu.SemaphoreType.REGULAR,
            pltpu.SemaphoreType.DMA((1,)),
            pltpu.SemaphoreType.DMA((chunks,)),
            pltpu.SemaphoreType.DMA((chunks,)),
            pltpu.SemaphoreType.DMA((max(1, chunks - 1),)),
            pltpu.SemaphoreType.DMA((max(1, chunks - 1),)),
            pltpu.VMEM((max(1, chunks - 1), distinct, TILE, width), half),
        ],
        compiler_params=pltpu.CompilerParams(
            collective_id=0, has_side_effects=True, vmem_limit_bytes=60 * 1024 * 1024
        ),
        name="step_and_gossip",
    )(hidden, grad_out, weight, moment, worker_of_slot.reshape(1, workers), round_shift)
    mixed, new_moment = pl.pallas_call(
        store,
        out_shape=[jax.ShapeDtypeStruct((rows, features), half)] * 2,
        in_specs=[anywhere, anywhere],
        out_specs=[anywhere, anywhere],
        scratch_shapes=[pltpu.SemaphoreType.DMA((2,))],
        name="store",
    )(
        pltpu.with_memory_space_constraint(mixed, pltpu.VMEM),
        pltpu.with_memory_space_constraint(new_moment, pltpu.VMEM),
    )
    return (mixed.reshape(weights.shape), new_moment.reshape(momentum.shape))


def solution(mesh):
    sizes = (mesh.shape["gx"], mesh.shape["gy"], mesh.shape["gz"])
    placed = (
        P("gz", "gy", "gx", None, None),
        P("gz", "gy", "gx", None, None),
        P("gz", "gy", "gx", None, None),
        P("gz", "gy", "gx", None, None),
        P(),
        P(),
    )
    return jax.shard_map(
        functools.partial(shards, sizes),
        mesh=mesh,
        in_specs=placed,
        out_specs=(P("gx", "gy", "gz", None, None), P("gz", "gy", "gx", None, None)),
        check_vma=False,
    )
```

```python
import functools

import jax
import jax.numpy as jnp
from jax import lax
from jax.experimental import pallas as pl
from jax.experimental.pallas import tpu as pltpu
from jax.sharding import PartitionSpec as P

learn_rate = 0.01
beta_keep = 0.9
TILE = 16
GROUP = 2
BANK = 4
LOGICAL = pl.DeviceIdType.LOGICAL


def iota(shape, axis):
    return lax.broadcasted_iota(jnp.int32, shape, axis)


def ones_where(mask):
    return jnp.where(mask, 1.0, 0.0).astype(jnp.bfloat16)


def exact_dot(a, b):
    return jnp.dot(a, b, preferred_element_type=jnp.float32)


def kernel(
    sizes,
    hidden_hbm,
    grad_hbm,
    weight_hbm,
    moment_hbm,
    held_hbm,
    shift_hbm,
    out_ref,
    new_moment_ref,
    hidden,
    grad_ref,
    weight,
    moment,
    held_ref,
    shift_ref,
    stage,
    recv,
    mixed,
    spread,
    load_sem,
    table_sem,
    line_sem,
    hub_sem,
    all_sem,
    sent_sem,
    recv_sem,
    back_recv_sem,
    far_recv_sem,
    forward_recv_sem,
    spare,
):
    size_x, size_y, size_z = sizes
    workers = size_x * size_y * size_z
    width = stage.shape[-1]
    groups, _, span = hidden.shape
    columns = stage.shape[1]
    parts = out_ref.shape[0] // TILE
    chunks = recv.shape[0]
    rounds = shift_ref.shape[0]
    my_x, my_y, my_z = lax.axis_index("gx"), lax.axis_index("gy"), lax.axis_index("gz")
    me = (my_x * size_y + my_y) * size_z + my_z
    slot = my_x + size_x * (my_y + size_y * my_z)

    plane = size_y * size_z
    half = workers // 2
    side = lax.div(me, half)
    lines = plane // GROUP
    layers = (half if columns == workers else columns) // plane
    my_line = lax.div(lax.rem(me, plane), GROUP)

    def ranked(step):
        far = 1 - lax.div(step, half)
        turn = (side ^ far) * (size_x - 1)
        layer = lax.div(lax.rem(step, half), plane) ^ turn
        turn_step = lax.rem(step, plane)
        low = ((me & (plane - 1)) ^ (plane - 1 - turn_step)) & (plane - 2)
        return layer * plane + low + (turn_step & 1)

    def pair(group):
        side_groups = layers * lines
        order = lax.rem(group, side_groups)
        turn = my_line ^ ((lines - lax.div(order, layers)) & (lines - 1))
        layer = lax.rem(order, layers)
        if columns == workers:
            far = 1 - lax.div(group, side_groups)
            layer = layer ^ my_x ^ (far * (size_x - 1))
        return layer * lines + turn

    def bank(group):
        return GROUP + lax.div(group + BANK - 2, BANK)

    def loads(group, first=0, count=GROUP, sem=None):
        place = pair(group)
        take = count * width
        cut = pl.ds(pl.multiple_of(place * span + first * width, 128), take)
        return [
            pltpu.make_async_copy(
                source.at[:, cut],
                kept.at[place, :, pl.ds(first * width, take)],
                load_sem.at[bank(group) if sem is None else sem],
            )
            for source, kept in (
                (hidden_hbm, hidden),
                (moment_hbm, moment),
                (weight_hbm, weight),
            )
        ]

    def load(group, carry):
        for copy in loads(group):
            copy.start()
        return carry

    def single(k):
        return loads(0, k, 1, k)

    barrier = pltpu.get_barrier_semaphore()
    hub = my_x == 0

    def signal(sem, device):
        pl.semaphore_signal(sem, inc=1, device_id=device, device_id_type=LOGICAL)

    def mirror(device):
        return device ^ ((size_x - 1) * plane)

    half_x = size_x // 2
    lead_x = side * (size_x - 1)
    right_lead = my_x == size_x - 1
    leader = jnp.logical_or(hub, right_lead)
    left_inner = jnp.logical_and(my_x > 0, my_x < half_x)
    right_inner = jnp.logical_and(my_x >= half_x, my_x < size_x - 1)
    lead = me ^ ((my_x ^ lead_x) * plane)

    def greet_side(step, carry):
        signal(barrier, me ^ ((step + 1) * plane))
        signal(barrier, me ^ ((step + 1) * plane) ^ 1)
        return carry

    def tell_side(step, carry):
        signal(line_sem, me ^ ((step + 1) * plane))
        return carry

    def greet():
        signal(barrier, mirror(me))
        signal(barrier, mirror(me) ^ 1)
        signal(barrier, me ^ 1)

        @pl.when(jnp.logical_not(leader))
        def _():
            signal(barrier, lead)
            signal(barrier, lead ^ 1)

        @pl.when(hub)
        def _():
            lax.fori_loop(0, half_x - 1, greet_side, 0)
            lax.fori_loop(0, lines - 1, greet_hub, 0)

    others = 2 * (half_x - 1)
    expected = 3 + jnp.where(leader, others, 0) + jnp.where(left_inner, 2, 0)
    expected = expected + jnp.where(hub, lines - 1, 0)

    def greet_hub(step, carry):
        signal(barrier, me ^ ((step + 1) * GROUP))
        return carry

    def tell_hub(step, carry):
        signal(hub_sem, me ^ ((step + 1) * GROUP))
        return carry

    def tell_line(step, carry):
        signal(all_sem, me ^ ((step + 1) * plane))
        return carry

    grad_copy = pltpu.make_async_copy(grad_hbm, grad_ref, load_sem.at[0])
    table_copies = [
        pltpu.make_async_copy(held_hbm, held_ref, table_sem.at[0]),
        pltpu.make_async_copy(shift_hbm, shift_ref, table_sem.at[0]),
    ]
    grad_copy.start()
    for copy in single(0):
        copy.start()
    greet()
    for k in range(1, GROUP):
        for copy in single(k):
            copy.start()
    lax.fori_loop(1, groups, load, 0)
    for copy in table_copies:
        copy.start()

    def place_of(part, where):
        block = part * columns
        return block // workers, block % workers + where

    def send(part, where):
        chunk, device = place_of(part, where)

        @pl.when(device != me)
        def _():
            pltpu.make_async_remote_copy(
                src_ref=stage.at[part, where],
                dst_ref=recv.at[chunk, slot],
                send_sem=sent_sem.at[0],
                recv_sem=recv_sem.at[chunk],
                device_id=device,
                device_id_type=LOGICAL,
            ).start()

    early = [part for part in range(parts) if place_of(part, 0)[0] == 0]
    late = [part for part in range(parts) if place_of(part, 0)[0] > 0]

    def advance(place, first, count):
        low, take = first * width, count * width
        kept = (place, slice(None), slice(low, low + take))
        velocity = beta_keep * moment[kept].astype(jnp.float32) + exact_dot(
            grad_ref[...], hidden[kept]
        )
        cut = pl.ds(pl.multiple_of(place * span + low, 128), take)
        new_moment_ref[:, cut] = velocity.astype(jnp.bfloat16)
        stepped = (weight[kept].astype(jnp.float32) - learn_rate * velocity).astype(
            jnp.bfloat16
        )
        for k in range(count):
            for part in range(parts):
                stage[part, place * GROUP + first + k] = stepped[
                    part * TILE : (part + 1) * TILE, k * width : (k + 1) * width
                ]

    def compute(group):
        @pl.when((group < 2) | (lax.rem(group + BANK - 2, BANK) == 0))
        def _():
            for step in range(BANK):

                @pl.when((bank(group + step) == bank(group)) & (group + step < groups))
                def _():
                    for copy in loads(group + step):
                        copy.wait()

        advance(pair(group), 0, GROUP)

    def compute_single(k):
        for copy in single(k):
            copy.wait()
        advance(pair(0), k, 1)

    def send_parts(which, group):
        for k in range(GROUP):
            for part in which:
                send(part, pair(group) * GROUP + k)

    def compute_ahead(group, carry):
        compute(group)
        return carry

    def send_ahead(group, carry):
        send_parts(early, group)
        return carry

    def compute_and_send(group, carry):
        compute(group)
        send_parts(early, group - 1)
        return carry

    def send_late(group, carry):
        send_parts(late, group)
        return carry

    grad_copy.wait()
    compute_single(0)
    pl.semaphore_wait(barrier, expected)

    @pl.when(left_inner)
    def _():
        signal(line_sem, lead)

    @pl.when(hub)
    def _():
        pl.semaphore_wait(line_sem, half_x - 1)

    @pl.when(leader)
    def _():
        lax.fori_loop(0, half_x - 1, tell_side, 0)

    @pl.when(hub)
    def _():
        lax.fori_loop(0, lines - 1, tell_hub, 0)

    def send_all(group):
        send_parts(early, jnp.int32(group))
        send_parts(late, jnp.int32(group))

    for k in range(GROUP):
        if k:
            compute_single(k)
        if columns == workers:
            for part in range(parts):
                send(part, pair(0) * GROUP + k)
    compute(jnp.int32(1))

    @pl.when(jnp.logical_not(leader))
    def _():
        pl.semaphore_wait(line_sem, 1)

    @pl.when(right_inner)
    def _():
        signal(line_sem, lead)

    @pl.when(right_lead)
    def _():
        pl.semaphore_wait(line_sem, half_x - 1)

    if half_x > 2:

        @pl.when(right_lead)
        def _():
            lax.fori_loop(0, half_x - 1, tell_side, 0)

        @pl.when(right_inner)
        def _():
            pl.semaphore_wait(line_sem, 1)

    if columns != workers:
        send_all(0)
    send_all(1)
    for group in range(2, layers):
        compute(jnp.int32(group))
        send_all(group)
    ahead = min(layers + 1, groups - 1)
    lax.fori_loop(layers, ahead, compute_ahead, 0)

    @pl.when(hub)
    def _():
        pl.semaphore_wait(hub_sem, lines - 1)
        lax.fori_loop(0, size_x - 1, tell_line, 0)

    @pl.when(jnp.logical_not(hub))
    def _():
        pl.semaphore_wait(all_sem, 1)

    lax.fori_loop(layers, ahead - 1, send_ahead, 0)
    lax.fori_loop(ahead, groups, compute_and_send, 0)
    send_parts(early, jnp.int32(groups - 1))
    if late:
        lax.fori_loop(layers, groups, send_late, 0)
    for chunk in range(chunks):
        block = chunk * workers + me
        recv[chunk, slot] = stage[lax.div(block, columns), lax.rem(block, columns)]
    for copy in table_copies:
        copy.wait()

    square = (workers, workers)
    gap = lax.rem(iota(square, 0) - iota(square, 1) + workers, workers)
    level = jnp.full(square, -1, jnp.int32)
    for power in range(workers.bit_length() - 1):
        level = jnp.where(gap == 1 << power, power, level)
    table = ones_where(held_ref[...] == iota(square, 0))
    for step in range(rounds):
        turn = ones_where((gap == 0) | (level == shift_ref[step]))
        table = exact_dot(turn, table).astype(jnp.bfloat16)
    distinct = workers // 2
    table = (table[:distinct].astype(jnp.float32) * 0.5**rounds).astype(jnp.bfloat16)
    wide = (workers, workers * TILE)
    table = exact_dot(table, ones_where(iota(wide, 1) // TILE == iota(wide, 0))).astype(
        jnp.bfloat16
    )
    height = min(256, distinct * TILE)

    def fill(step, carry):
        tall = (height, distinct)
        pick = ones_where((iota(tall, 0) + step * height) // TILE == iota(tall, 1))
        full = (height, workers * TILE)
        same = iota(full, 0) % TILE == iota(full, 1) % TILE
        spread[pl.ds(pl.multiple_of(step * height, height), height), :] = jnp.where(
            same, exact_dot(pick, table), 0.0
        ).astype(jnp.bfloat16)
        return carry

    lax.fori_loop(0, distinct * TILE // height, fill, 0)

    def pieces_wait(sem, count=workers - 1):
        ref = recv.at[0, pl.ds(0, count)]
        pltpu.make_async_copy(ref, ref, sem).wait()

    def home(chunk, owner):
        block = chunk * workers + owner
        row = pl.multiple_of(lax.div(block, columns) * TILE, TILE)
        first = pl.multiple_of(lax.rem(block, columns) * width, 128)
        return pl.ds(row, TILE), pl.ds(first, width)

    mine = lax.rem(me, half)
    def forward_all(chunk):
        pieces_wait(far_recv_sem.at[chunk], half - 1)

        def forward(step, carry):
            owner = ranked(step ^ 1)

            @pl.when(owner != mirror(me))
            def _():
                pltpu.make_async_remote_copy(
                    src_ref=out_ref.at[home(chunk, owner)],
                    dst_ref=spare.at[chunk, mine],
                    send_sem=sent_sem.at[0],
                    recv_sem=forward_recv_sem.at[chunk],
                    device_id=mirror(owner),
                    device_id_type=LOGICAL,
                ).start()

            return carry

        lax.fori_loop(0, half, forward, 0)
        spare[chunk, mine] = jnp.zeros((TILE, width), jnp.bfloat16)

    for chunk in range(chunks):
        pieces_wait(recv_sem.at[chunk])
        got = recv[chunk].reshape(workers * TILE, width)

        def blend(step, carry):
            result = exact_dot(
                spread[pl.ds(pl.multiple_of(step * height, height), height), :], got
            )
            mixed[chunk, pl.ds(step * (height // TILE), height // TILE)] = result.astype(
                jnp.bfloat16
            ).reshape(height // TILE, TILE, width)
            return carry

        lax.fori_loop(0, distinct * TILE // height, blend, 0)
        out_ref[home(chunk, me)] = mixed[chunk, mine]

        def back(step, absent, sem):
            device = ranked(step)

            @pl.when(device != absent)
            def _():
                pltpu.make_async_remote_copy(
                    src_ref=mixed.at[chunk, lax.rem(device, half)],
                    dst_ref=out_ref.at[home(chunk, me)],
                    send_sem=sent_sem.at[0],
                    recv_sem=sem.at[chunk],
                    device_id=device,
                    device_id_type=LOGICAL,
                ).start()

        def back_far(step, carry):
            last = chunk == chunks - 1
            back(step, me if last else mirror(me), back_recv_sem if last else far_recv_sem)
            return carry

        def back_near(step, carry):
            back(step, me, back_recv_sem)
            return carry

        if chunk == chunks - 1:
            lax.fori_loop(0, half // 2, back_far, 0)
            lax.fori_loop(half, workers, back_near, 0)
            for earlier in range(chunks - 1):
                forward_all(earlier)
            lax.fori_loop(half // 2, half, back_far, 0)
        else:
            lax.fori_loop(half, workers, back_near, 0)
            lax.fori_loop(0, half, back_far, 0)

    for chunk in range(chunks - 1):
        pieces_wait(forward_recv_sem.at[chunk], half - 1)
        total = jnp.zeros((TILE, width), jnp.float32)
        for k in range(half):
            piece = spare[chunk, k].astype(jnp.float32)
            total = total - piece if k % 2 else total + piece
        total = jnp.where(lax.rem(me, 2) == 1, total, -total)
        out_ref[home(chunk, mirror(me))] = total.astype(jnp.bfloat16)

    for chunk in range(chunks):
        last = chunk == chunks - 1
        for count in (workers - 1, workers - 1 if last else workers - 2):
            pieces_wait(sent_sem.at[0], count)
        if not last:
            pieces_wait(sent_sem.at[0], half - 1)
        pieces_wait(back_recv_sem.at[chunk], workers - 1 if last else half - 1)


def store(mixed_ref, moment_ref, mixed_hbm, moment_hbm, sem):
    copies = [
        pltpu.make_async_copy(mixed_ref, mixed_hbm, sem.at[0]),
        pltpu.make_async_copy(moment_ref, moment_hbm, sem.at[1]),
    ]
    for copy in copies:
        copy.start()
    for copy in copies:
        copy.wait()


def shards(sizes, hidden_acts, output_grad, weights, momentum, worker_of_slot, round_shift):
    hidden = hidden_acts.reshape(hidden_acts.shape[-2:])
    grad_out = output_grad.reshape(output_grad.shape[-2:]).T
    weight = weights.reshape(weights.shape[-2:])
    moment = momentum.reshape(momentum.shape[-2:])
    workers = sizes[0] * sizes[1] * sizes[2]
    tokens, features = hidden.shape
    rows = weight.shape[0]
    parts = rows // TILE
    width = max(128, features // workers)
    columns = features // width
    chunks = parts * columns // workers
    distinct = workers // 2
    groups = columns // GROUP
    anywhere = pl.BlockSpec(memory_space=pl.ANY)
    vmem = pl.BlockSpec(memory_space=pltpu.VMEM)
    half = jnp.bfloat16
    mixed, new_moment = pl.pallas_call(
        functools.partial(kernel, sizes),
        out_shape=[pltpu.VMEM((rows, features), half)] * 2,
        in_specs=[anywhere] * 6,
        out_specs=[vmem, vmem],
        scratch_shapes=[
            pltpu.VMEM((groups, tokens, GROUP * width), half),
            pltpu.VMEM((rows, tokens), half),
            pltpu.VMEM((groups, rows, GROUP * width), half),
            pltpu.VMEM((groups, rows, GROUP * width), half),
            pltpu.VMEM((1, workers), jnp.int32),
            pltpu.SMEM(round_shift.shape, jnp.int32),
            pltpu.VMEM((parts, columns, TILE, width), half),
            pltpu.VMEM((chunks, workers, TILE, width), half),
            pltpu.VMEM((chunks, distinct, TILE, width), half),
            pltpu.VMEM((distinct * TILE, workers * TILE), half),
            pltpu.SemaphoreType.DMA((GROUP + 1 + pl.cdiv(groups - 2, BANK),)),
            pltpu.SemaphoreType.DMA((1,)),
            pltpu.SemaphoreType.REGULAR,
            pltpu.SemaphoreType.REGULAR,
            pltpu.SemaphoreType.REGULAR,
            pltpu.SemaphoreType.DMA((1,)),
            pltpu.SemaphoreType.DMA((chunks,)),
            pltpu.SemaphoreType.DMA((chunks,)),
            pltpu.SemaphoreType.DMA((max(1, chunks - 1),)),
            pltpu.SemaphoreType.DMA((max(1, chunks - 1),)),
            pltpu.VMEM((max(1, chunks - 1), distinct, TILE, width), half),
        ],
        compiler_params=pltpu.CompilerParams(
            collective_id=0, has_side_effects=True, vmem_limit_bytes=60 * 1024 * 1024
        ),
        name="step_and_gossip",
    )(hidden, grad_out, weight, moment, worker_of_slot.reshape(1, workers), round_shift)
    mixed, new_moment = pl.pallas_call(
        store,
        out_shape=[jax.ShapeDtypeStruct((rows, features), half)] * 2,
        in_specs=[anywhere, anywhere],
        out_specs=[anywhere, anywhere],
        scratch_shapes=[pltpu.SemaphoreType.DMA((2,))],
        name="store",
    )(
        pltpu.with_memory_space_constraint(mixed, pltpu.VMEM),
        pltpu.with_memory_space_constraint(new_moment, pltpu.VMEM),
    )
    return (mixed.reshape(weights.shape), new_moment.reshape(momentum.shape))


def solution(mesh):
    sizes = (mesh.shape["gx"], mesh.shape["gy"], mesh.shape["gz"])
    placed = (
        P("gz", "gy", "gx", None, None),
        P("gz", "gy", "gx", None, None),
        P("gz", "gy", "gx", None, None),
        P("gz", "gy", "gx", None, None),
        P(),
        P(),
    )
    return jax.shard_map(
        functools.partial(shards, sizes),
        mesh=mesh,
        in_specs=placed,
        out_specs=(P("gx", "gy", "gz", None, None), P("gz", "gy", "gx", None, None)),
        check_vma=False,
    )
```
